512 devices in a mesh: sweep: 2 (over y), tm: 128 (over x, z), unit: 2 (over core).
Axes of the slice: x: 8, y: 2, z: 16, core: 2. Of those that a mesh axis runs over, the one named last changes fastest.
The devices are a block of a 8x8x16 slice.
Arguments:
- projections: bfloat16 [2, 512, 3, 1024], P('sweep', 'tm', None, 'unit'), parts along dimension 0, may hold values from -6 to 6
- recurrent: bfloat16 [2048, 3, 1024], P('sweep', None, 'unit'), parts along dimension 0, may hold values from -0.375 to 0.375
- update_bias: float32 [2048], P(('sweep', 'unit')), parts along dimension 0, may hold values from -1 to 13
- candidate_bias: float32 [2048], P(('sweep', 'unit')), parts along dimension 0, may hold values from -5 to 5
- start_state: float32 [2, 1024], P('sweep', 'unit'), parts along dimension 0, may hold values from -4 to 4
- initial_guess: float32 [2, 512, 1024], P('sweep', 'tm', 'unit'), parts along dimension 0, may hold values from -3 to 3
Outputs:
- trajectory: float32 [2, 512, 1024], P('sweep', 'tm', 'unit'), parts along dimension 0
The draws below stay inside these ranges and needn't reach their ends.
There are 2 independent parts, one for each index of `sweep`. The reference program is written for one: setup_inputs(seed, part) draws one part's arguments, and reference() takes and returns one part's arrays. A program takes and returns all parts, laid end to end along the dimension named above; each array names one. Nothing has to cross between parts.
All inputs are finite; a program needn't handle non-finite values.
Results may differ from the reference program's by a relative error of at most 0.0017.
Values may be sent and summed in bfloat16 or wider, within the bound.
No kernel may reach another device: no remote copies, remote signals or barrier semaphores. Data moves between devices by JAX's collectives and lax.ppermute only.
A program may use at most 64 MiB of HBM per device.

```python
import jax
import jax.numpy as jnp
from jax import lax

H = 1024
BLOCK = 128
BATCH = 1
NEWTON = 2
LENGTH = 512


def draw_update_bias(key, part):
    first_key = jax.random.fold_in(key, 11)
    second_key = jax.random.fold_in(key, 23)
    third_key = jax.random.fold_in(key, 37)
    quick_bias = jax.random.uniform(first_key, (H,), jnp.float32, -1.0, 4.0)
    slow_bias = jax.random.uniform(second_key, (H,), jnp.float32, 10.0, 13.0)
    slow_share = 0.25
    chosen = jax.random.uniform(third_key, (H,), jnp.float32) < slow_share
    return jnp.where(chosen, slow_bias, quick_bias).astype(jnp.float32)


def block_levels(key, shape, cuts, low, high):
    gain = 1.0
    for dim, shards_of in cuts:
        heights = jax.random.uniform(jax.random.fold_in(jax.random.fold_in(key, 6), dim), (shards_of,), jnp.float32, low / len(cuts), high / len(cuts))
        gain = gain * jnp.repeat(jnp.exp(heights), shape[dim] // shards_of).reshape((-1,) + (1,) * (len(shape) - 1 - dim))
    return gain


def scatter_about(key, extent, scale, limit, split=(), kind=jnp.bfloat16):
    values = scale * jax.random.normal(key, extent, jnp.float32)
    if split:
        values = values * block_levels(key, extent, split, -0.22, 0.18)
    return jnp.clip(values, -limit, limit).astype(kind)


def setup_inputs(seed: int = 0, part: int = 0) -> dict:
    key_of = jax.random.split(jax.random.key(seed), 7)
    own_keys = jax.random.split(jax.random.fold_in(key_of[6], part), 7)
    projections = scatter_about(own_keys[0], (BATCH, LENGTH, 3, H), 1.0, 6.0, ((1, 128), (3, 2)))
    recurrent = scatter_about(own_keys[1], (H, 3, H), (H // 4) ** -0.5, 0.375, ((2, 2),))
    update_bias = draw_update_bias(jax.random.fold_in(jax.random.fold_in(key_of[6], part), 71), part)
    candidate_bias = scatter_about(own_keys[3], (H,), 1.0, 5.0, ((0, 2),), jnp.float32)
    start_state = scatter_about(own_keys[4], (BATCH, H), 0.7, 4.0, ((1, 2),), jnp.float32)
    initial_guess = scatter_about(own_keys[5], (BATCH, LENGTH, H), 0.5, 3.0, ((1, 128), (2, 2)), jnp.float32)
    return {"projections": projections, "recurrent": recurrent, "update_bias": update_bias, "candidate_bias": candidate_bias, "start_state": start_state, "initial_guess": initial_guess}


def jacobian_apply(vector, update_gate, coef_a, coef_c, coef_d, blocks):
    lead_shape = vector.shape[:-1]
    grouped = vector.reshape(lead_shape + (H // BLOCK, BLOCK))
    block_terms = jnp.einsum("...ki,kigj->...gkj", grouped, blocks, precision=lax.Precision.HIGHEST)
    block_terms = block_terms.reshape(lead_shape + (3, H))
    return (update_gate * vector + coef_a * block_terms[..., 0, :]
            + coef_c * block_terms[..., 1, :] + coef_d * block_terms[..., 2, :])


def reference(projections, recurrent, update_bias, candidate_bias, start_state, initial_guess):
    blocks = recurrent.astype(jnp.float32).reshape(H // BLOCK, BLOCK, 3, H // BLOCK, BLOCK)
    blocks = jnp.einsum("kigkj->kigj", blocks)
    flat_weight = recurrent.reshape(H, 3 * H)
    trajectory = initial_guess
    for newton_turn in range(NEWTON):
        previous = jnp.concatenate([start_state[:, None, :], trajectory[:, :-1, :]], axis=1)
        panels = previous.astype(jnp.bfloat16).reshape(BATCH * LENGTH, H)
        recurrent_terms = jnp.dot(panels, flat_weight, preferred_element_type=jnp.float32)
        recurrent_terms = recurrent_terms.reshape(BATCH, LENGTH, 3, H)
        update_gate = jax.nn.sigmoid(projections[:, :, 0].astype(jnp.float32) + recurrent_terms[:, :, 0] + update_bias)
        reset_gate = jax.nn.sigmoid(projections[:, :, 1].astype(jnp.float32) + recurrent_terms[:, :, 1])
        cand_rec = recurrent_terms[:, :, 2] + candidate_bias
        candidate = jnp.tanh(projections[:, :, 2].astype(jnp.float32) + reset_gate * cand_rec)
        mapped = (1.0 - update_gate) * candidate + update_gate * previous
        coef_a = (previous - candidate) * update_gate * (1.0 - update_gate)
        coef_d = (1.0 - update_gate) * (1.0 - candidate * candidate) * reset_gate
        coef_c = coef_d * cand_rec * (1.0 - reset_gate)
        offsets = mapped - jacobian_apply(previous, update_gate, coef_a, coef_c, coef_d, blocks)

        def advance(current, inputs):
            gate_step, a_step, c_step, d_step, offset_step = inputs
            following = jacobian_apply(current, gate_step, a_step, c_step, d_step, blocks) + offset_step
            return following, following

        sequence_inputs = tuple(jnp.transpose(item, (1, 0, 2)) for item in (update_gate, coef_a, coef_c, coef_d, offsets))
        carried, states = lax.scan(advance, start_state, sequence_inputs)
        trajectory = jnp.transpose(states, (1, 0, 2))
    return trajectory
```

```python
import functools

import jax
import jax.numpy as jnp
from jax import lax
from jax.experimental import pallas as pl
from jax.experimental.pallas import tpu as pltpu
from jax.sharding import Mesh
from jax.sharding import PartitionSpec as P

BLOCK = 128
GROUPS = 8
TM = ("x", "zh", "zl")
Z = ("zh", "zl")
INTERPRET = False
ROWS = BLOCK + 16
F32 = jnp.float32
BF16 = jnp.bfloat16


def split2(value):
    high = value.astype(BF16)
    low = (value - high.astype(F32)).astype(BF16)
    return high, low


def split3(value):
    high = value.astype(BF16)
    rest = value - high.astype(F32)
    mid = rest.astype(BF16)
    low = (rest - mid.astype(F32)).astype(BF16)
    return high, mid, low


def dot(left, right):
    return jnp.dot(left, right, preferred_element_type=F32)


def gates(rec, proj, prev, guess, ub_ref, cb_ref, par_ref):
    update = jax.nn.sigmoid(proj[0] + rec[:, 0:BLOCK] + ub_ref[...])
    reset = jax.nn.sigmoid(proj[1] + rec[:, BLOCK : 2 * BLOCK])
    inner = rec[:, 2 * BLOCK : 3 * BLOCK] + cb_ref[...]
    cand = jnp.tanh(proj[2] + reset * inner)
    mapped = (1.0 - update) * cand + update * prev
    full = (1.0 - update) * (1.0 - cand * cand) * reset
    par_ref[0] = update
    par_ref[1] = (prev - cand) * update * (1.0 - update)
    par_ref[2] = full * inner * (1.0 - reset)
    par_ref[3] = full
    par_ref[4] = mapped - guess


def advance(value, terms, rows):
    u, a, c, d = rows
    return (
        u * value
        + a * terms[:, 0:BLOCK]
        + c * terms[:, BLOCK : 2 * BLOCK]
        + d * terms[:, 2 * BLOCK : 3 * BLOCK]
    )


def advance_rows(value, double, par_ref, low, high):
    terms = dot(jnp.concatenate(split2(value), axis=1), double)
    rows = [par_ref[i, low:high, :] for i in range(4)]
    return advance(value, terms, rows) + par_ref[4, low:high, :]


def compose_all(par_ref, weight, maps_ref, send_ref, chunks, steps):
    eye = lax.broadcasted_iota(jnp.int32, (BLOCK, BLOCK), 0) == lax.broadcasted_iota(
        jnp.int32, (BLOCK, BLOCK), 1
    )
    wide = weight.astype(F32)
    double = jnp.concatenate([weight, weight], axis=0)
    part = 4
    for first in range(0, chunks, part):
        members = range(first, first + part)

        def rows_of(step, c):
            return [par_ref[i, step * chunks + c : step * chunks + c + 1, :] for i in range(4)]

        current = []
        for c in members:
            u, a, c_, d = rows_of(0, c)
            start = a * wide[:, 0:BLOCK] + c_ * wide[:, BLOCK : 2 * BLOCK] + d * wide[:, 2 * BLOCK :]
            current.append(start + jnp.where(eye, u, 0.0))
        for step in range(1, steps):
            stacked = jnp.concatenate([m.astype(BF16) for m in current], axis=0)
            terms = dot(stacked, weight)
            current = [
                advance(m, terms[k * BLOCK : (k + 1) * BLOCK], rows_of(step, c))
                for k, (m, c) in enumerate(zip(current, members))
            ]
        for m, c in zip(current, members):
            maps_ref[c, 0:BLOCK, :] = m
    vector = par_ref[4, 0:chunks, :]
    for step in range(1, steps):
        vector = advance_rows(vector, double, par_ref, step * chunks, (step + 1) * chunks)
    pad = jnp.zeros((ROWS - BLOCK - 1, BLOCK), F32)
    for c in range(chunks):
        maps_ref[c, BLOCK:ROWS, :] = jnp.concatenate([vector[c : c + 1], pad], axis=0)
    width = 1
    while width < chunks:
        for left in range(width - 1, chunks, 2 * width):
            before = jnp.concatenate(split2(maps_ref[left]), axis=1)
            for right in range(left + 1, left + 1 + width):
                high, low = split2(maps_ref[right, 0:BLOCK, :])
                upper = jnp.concatenate([high, low], axis=1)
                under = jnp.concatenate([high, jnp.zeros_like(low)], axis=1)
                both = dot(before, jnp.concatenate([upper, under], axis=0))
                both = both[:, 0:BLOCK] + both[:, BLOCK:]
                maps_ref[right, 0:BLOCK, :] = both[0:BLOCK]
                maps_ref[right, BLOCK:ROWS, :] = both[BLOCK:] + maps_ref[right, BLOCK:ROWS, :]
        width *= 2
    matrix = maps_ref[chunks - 1, 0:BLOCK, :]
    diagonal = jnp.sum(jnp.where(eye, matrix, 0.0), axis=0, keepdims=True)
    tail = [p.astype(F32) for p in split3(diagonal)]
    tail += [p.astype(F32) for p in split3(maps_ref[chunks - 1, BLOCK : BLOCK + 1, :])]
    tail.append(jnp.zeros((ROWS - BLOCK - 6, BLOCK), F32))
    matrix = jnp.where(eye, 0.0, matrix).astype(BF16)
    tail = jnp.concatenate(tail, axis=0).astype(BF16)
    for peer in range(send_ref.shape[0]):
        send_ref[peer, 0:BLOCK, :] = matrix
        send_ref[peer, BLOCK:ROWS, :] = tail


def first_maps(
    index_ref, own_ref, other_ref, w_ref, ub_ref, cb_ref,
    send_ref, maps_ref, par_ref, prev_ref, guess_ref, *, chunks, steps, blocks, stride,
):
    unit, place = index_ref[0], index_ref[1]

    def rows(ref, start):
        return ref[pl.ds(start, chunks, stride=stride), :]

    def all_steps(ref, start, jump=1):
        return jnp.concatenate([rows(ref, start + jump * s) for s in range(steps)], axis=0)

    half = blocks * BLOCK
    total = 0.0
    for ref, side in ((own_ref, unit), (other_ref, 1 - unit)):
        panels = [all_steps(ref, k * (steps + 1)).astype(BF16) for k in range(blocks)]
        columns = w_ref[pl.ds(pl.multiple_of(side * half, half), half), :]
        total = total + dot(jnp.concatenate(panels, axis=1), columns)
    base = blocks * (steps + 1)
    proj = [all_steps(own_ref, base + g, 3) for g in range(3)]
    prev = all_steps(own_ref, place * (steps + 1))
    guess = all_steps(own_ref, place * (steps + 1) + 1)
    prev_ref[...] = prev
    guess_ref[...] = guess
    gates(total, proj, prev, guess, ub_ref, cb_ref, par_ref)
    here = pl.multiple_of((unit * blocks + place) * BLOCK, BLOCK)
    compose_all(par_ref, w_ref[pl.ds(here, BLOCK), :], maps_ref, send_ref, chunks, steps)


def next_maps(
    index_ref, panel_ref, own_ref, prev_ref, guess_ref, w_ref, ub_ref, cb_ref,
    send_ref, maps_ref, par_ref, *, chunks, steps, blocks, stride,
):
    unit, place = index_ref[0], index_ref[1]
    sides = panel_ref.shape[0] // blocks
    panels = [panel_ref[k * sides + side] for side in range(sides) for k in range(blocks)]
    total = dot(jnp.concatenate(panels, axis=1), w_ref[...])
    base = blocks * (steps + 1)

    def all_steps(start):
        parts = [own_ref[pl.ds(start + 3 * s, chunks, stride=stride), :] for s in range(steps)]
        return jnp.concatenate(parts, axis=0)

    proj = [all_steps(base + g) for g in range(3)]
    gates(total, proj, prev_ref[...], guess_ref[...], ub_ref, cb_ref, par_ref)
    here = pl.multiple_of((unit * blocks + place) * BLOCK, BLOCK)
    compose_all(par_ref, w_ref[pl.ds(here, BLOCK), :], maps_ref, send_ref, chunks, steps)


def solve(index_ref, got_ref, maps_ref, par_ref, w_ref, chunks, steps, blocks):
    unit, place, group = index_ref[0], index_ref[1], index_ref[2]

    def pass_group(k, delta):
        block = got_ref[k]
        matrix = block[0:BLOCK]
        tail = block[BLOCK:ROWS].astype(F32)
        diagonal = tail[0:1] + tail[1:2] + tail[2:3]
        vector = tail[3:4] + tail[4:5] + tail[5:6]
        terms = dot(
            jnp.concatenate(split2(delta), axis=1), jnp.concatenate([matrix, matrix], axis=0)
        )
        return terms + delta * diagonal + vector

    delta = lax.fori_loop(0, group, pass_group, jnp.zeros((16, BLOCK), F32))
    column = jnp.transpose(jnp.broadcast_to(delta[0:1], (BLOCK, BLOCK)))
    entries = [delta[0:1]]
    for c in range(chunks - 1):
        through = jnp.sum(column * maps_ref[c, 0:BLOCK, :], axis=0, keepdims=True)
        entries.append(through + maps_ref[c, BLOCK : BLOCK + 1, :])
    entries = jnp.concatenate(entries, axis=0)
    here = pl.multiple_of((unit * blocks + place) * BLOCK, BLOCK)
    weight = w_ref[pl.ds(here, BLOCK), :]
    double = jnp.concatenate([weight, weight], axis=0)
    current, after = entries, []
    for step in range(steps):
        current = advance_rows(current, double, par_ref, step * chunks, (step + 1) * chunks)
        after.append(current)
    return entries, after


def first_states(
    index_ref, got_ref, maps_ref, par_ref, w_ref, prev_ref, guess_ref,
    send_ref, prev_out, guess_out, *, chunks, steps, blocks,
):
    entries, after = solve(index_ref, got_ref, maps_ref, par_ref, w_ref, chunks, steps, blocks)
    prev = prev_ref[...] + jnp.concatenate([entries] + after[:-1], axis=0)
    prev_out[...] = prev
    guess_out[...] = guess_ref[...] + jnp.concatenate(after, axis=0)
    panel = prev.astype(BF16)
    for peer in range(send_ref.shape[0]):
        send_ref[peer] = panel


def last_states(
    index_ref, got_ref, maps_ref, par_ref, w_ref, guess_ref,
    send_ref, state_ref, *, chunks, steps, blocks,
):
    quarter = index_ref[3]
    _, after = solve(index_ref, got_ref, maps_ref, par_ref, w_ref, chunks, steps, blocks)
    state_ref[...] = guess_ref[...] + jnp.concatenate(after, axis=0)
    near = send_ref.shape[0]
    for peer in range(near):
        for step in range(steps):
            row = step * chunks + quarter * near + peer
            send_ref[peer, step : step + 1, :] = state_ref[pl.ds(row, 1), :]


SMEM = pl.BlockSpec(memory_space=pltpu.SMEM)
VMEM = pl.BlockSpec(memory_space=pltpu.VMEM)


def call(body, outs, args, scratch=()):
    return pl.pallas_call(
        body,
        out_shape=[jax.ShapeDtypeStruct(shape, kind) for shape, kind in outs],
        in_specs=[SMEM] + [VMEM] * (len(args) - 1),
        out_specs=[VMEM] * len(outs),
        scratch_shapes=list(scratch),
        compiler_params=pltpu.CompilerParams(vmem_limit_bytes=24 * 1024 * 1024),
        interpret=INTERPRET,
    )(*args)


def shards(projections, recurrent, update_bias, candidate_bias, start_state, initial_guess):
    _, steps, _, width_dev = projections.shape
    full_width = recurrent.shape[0]
    blocks = width_dev // BLOCK
    chunks = lax.axis_size(Z)
    near = lax.axis_size("zl")
    sides = lax.axis_size("unit")
    groups = lax.axis_size("x")
    total_steps = chunks * steps
    place = lax.axis_index("zl")
    unit = lax.axis_index("unit")
    group = lax.axis_index("x")
    index = jnp.stack([unit, place, group, lax.axis_index("zh")]).astype(jnp.int32)

    count = lax.axis_size(TM)
    last = lax.ppermute(
        initial_guess[:, -1, :], TM, [(source, source + 1) for source in range(count - 1)]
    )
    weight = lax.dynamic_slice_in_dim(recurrent, place * BLOCK, BLOCK, 2)
    weight = jnp.concatenate([weight[:, g, :] for g in range(3)], axis=1)
    bias_u = lax.dynamic_slice_in_dim(update_bias, place * BLOCK, BLOCK, 0)[None]
    bias_c = lax.dynamic_slice_in_dim(candidate_bias, place * BLOCK, BLOCK, 0)[None]

    entering = jnp.where(lax.axis_index(TM) == 0, start_state, last)
    states = jnp.concatenate([entering, initial_guess[0]], axis=0)
    states = jnp.transpose(states.reshape(steps + 1, blocks, BLOCK), (1, 0, 2))
    states = states.reshape(blocks * (steps + 1), BLOCK)
    inputs = jnp.transpose(projections[0].reshape(steps * 3, blocks, BLOCK), (1, 0, 2))
    payload = jnp.concatenate(
        [jnp.broadcast_to(states, (blocks, *states.shape)), inputs.astype(F32)], axis=1
    )
    stride = payload.shape[1]
    payload = jnp.broadcast_to(payload, (chunks // blocks, *payload.shape))
    payload = payload.reshape(chunks, stride, BLOCK)
    own = lax.all_to_all(payload, Z, split_axis=0, concat_axis=0, tiled=True)
    other = lax.ppermute(own, "unit", [(s, sides - 1 - s) for s in range(sides)])
    own = own.reshape(chunks * stride, BLOCK)
    other = other.reshape(chunks * stride, BLOCK)

    sizes = dict(chunks=chunks, steps=steps, blocks=blocks)
    maps_out = [
        ((groups, ROWS, BLOCK), BF16),
        ((chunks, ROWS, BLOCK), F32),
        ((5, total_steps, BLOCK), F32),
    ]
    rows_out = [((total_steps, BLOCK), F32)] * 2
    send, maps, params, prev, guess = call(
        functools.partial(first_maps, stride=stride, **sizes),
        maps_out + rows_out,
        (index, own, other, weight, bias_u, bias_c),
    )
    got = lax.all_to_all(send, "x", split_axis=0, concat_axis=0, tiled=True)
    send, prev, guess = call(
        functools.partial(first_states, **sizes),
        [((near * sides, total_steps, BLOCK), BF16)] + rows_out,
        (index, got, maps, params, weight, prev, guess),
    )
    panels = lax.all_to_all(send, ("zl", "unit"), split_axis=0, concat_axis=0, tiled=True)
    send, maps, params = call(
        functools.partial(next_maps, stride=stride, **sizes),
        maps_out,
        (index, panels, own, prev, guess, weight, bias_u, bias_c),
    )
    got = lax.all_to_all(send, "x", split_axis=0, concat_axis=0, tiled=True)
    (send,) = call(
        functools.partial(last_states, **sizes),
        [((near, steps, BLOCK), F32)],
        (index, got, maps, params, weight, guess),
        [pltpu.VMEM((total_steps, BLOCK), F32)],
    )
    final = lax.all_to_all(send, "zl", split_axis=0, concat_axis=0, tiled=True)
    return jnp.transpose(final, (1, 0, 2)).reshape(1, steps, width_dev)


def solution(mesh):
    count = mesh.shape["tm"]
    near = 4
    finer = Mesh(
        mesh.devices.reshape(
            mesh.shape["sweep"], GROUPS, count // GROUPS // near, near, mesh.shape["unit"]
        ),
        ("sweep", "x", "zh", "zl", "unit"),
    )
    return jax.shard_map(
        shards,
        mesh=finer,
        in_specs=(
            P("sweep", TM, None, "unit"),
            P("sweep", None, "unit"),
            P(("sweep", "unit")),
            P(("sweep", "unit")),
            P("sweep", "unit"),
            P("sweep", TM, "unit"),
        ),
        out_specs=P("sweep", TM, "unit"),
        check_vma=False,
    )
```

```python
import functools

import jax
import jax.numpy as jnp
from jax import lax
from jax.experimental import pallas as pl
from jax.experimental.pallas import tpu as pltpu
from jax.sharding import Mesh
from jax.sharding import PartitionSpec as P

BLOCK = 128
GROUPS = 8
TM = ("x", "zh", "zl")
Z = ("zh", "zl")
INTERPRET = False
ROWS = BLOCK + 16
F32 = jnp.float32
BF16 = jnp.bfloat16


def split2(value):
    high = value.astype(BF16)
    low = (value - high.astype(F32)).astype(BF16)
    return high, low


def split3(value):
    high = value.astype(BF16)
    rest = value - high.astype(F32)
    mid = rest.astype(BF16)
    low = (rest - mid.astype(F32)).astype(BF16)
    return high, mid, low


def dot(left, right):
    return jnp.dot(left, right, preferred_element_type=F32)


def gates(rec, proj, prev, guess, ub_ref, cb_ref, par_ref):
    update = jax.nn.sigmoid(proj[0] + rec[:, 0:BLOCK] + ub_ref[...])
    reset = jax.nn.sigmoid(proj[1] + rec[:, BLOCK : 2 * BLOCK])
    inner = rec[:, 2 * BLOCK : 3 * BLOCK] + cb_ref[...]
    cand = jnp.tanh(proj[2] + reset * inner)
    mapped = (1.0 - update) * cand + update * prev
    full = (1.0 - update) * (1.0 - cand * cand) * reset
    par_ref[0] = update
    par_ref[1] = (prev - cand) * update * (1.0 - update)
    par_ref[2] = full * inner * (1.0 - reset)
    par_ref[3] = full
    par_ref[4] = mapped - guess


def advance(value, terms, rows):
    u, a, c, d = rows
    return (
        u * value
        + a * terms[:, 0:BLOCK]
        + c * terms[:, BLOCK : 2 * BLOCK]
        + d * terms[:, 2 * BLOCK : 3 * BLOCK]
    )


def advance_rows(value, double, par_ref, low, high):
    terms = dot(jnp.concatenate(split2(value), axis=1), double)
    rows = [par_ref[i, low:high, :] for i in range(4)]
    return advance(value, terms, rows) + par_ref[4, low:high, :]


def compose_all(par_ref, weight, maps_ref, send_ref, chunks, steps):
    eye = lax.broadcasted_iota(jnp.int32, (BLOCK, BLOCK), 0) == lax.broadcasted_iota(
        jnp.int32, (BLOCK, BLOCK), 1
    )
    wide = weight.astype(F32)
    double = jnp.concatenate([weight, weight], axis=0)
    part = 4
    for first in range(0, chunks, part):
        members = range(first, first + part)

        def rows_of(step, c):
            return [par_ref[i, step * chunks + c : step * chunks + c + 1, :] for i in range(4)]

        current = []
        for c in members:
            u, a, c_, d = rows_of(0, c)
            start = a * wide[:, 0:BLOCK] + c_ * wide[:, BLOCK : 2 * BLOCK] + d * wide[:, 2 * BLOCK :]
            current.append(start + jnp.where(eye, u, 0.0))
        for step in range(1, steps):
            stacked = jnp.concatenate([m.astype(BF16) for m in current], axis=0)
            terms = dot(stacked, weight)
            current = [
                advance(m, terms[k * BLOCK : (k + 1) * BLOCK], rows_of(step, c))
                for k, (m, c) in enumerate(zip(current, members))
            ]
        for m, c in zip(current, members):
            maps_ref[c, 0:BLOCK, :] = m
    vector = par_ref[4, 0:chunks, :]
    for step in range(1, steps):
        vector = advance_rows(vector, double, par_ref, step * chunks, (step + 1) * chunks)
    pad = jnp.zeros((ROWS - BLOCK - 1, BLOCK), F32)
    for c in range(chunks):
        maps_ref[c, BLOCK:ROWS, :] = jnp.concatenate([vector[c : c + 1], pad], axis=0)
    width = 1
    while width < chunks:
        for left in range(width - 1, chunks, 2 * width):
            before = jnp.concatenate(split2(maps_ref[left]), axis=1)
            for right in range(left + 1, left + 1 + width):
                high, low = split2(maps_ref[right, 0:BLOCK, :])
                upper = jnp.concatenate([high, low], axis=1)
                under = jnp.concatenate([high, jnp.zeros_like(low)], axis=1)
                both = dot(before, jnp.concatenate([upper, under], axis=0))
                both = both[:, 0:BLOCK] + both[:, BLOCK:]
                maps_ref[right, 0:BLOCK, :] = both[0:BLOCK]
                maps_ref[right, BLOCK:ROWS, :] = both[BLOCK:] + maps_ref[right, BLOCK:ROWS, :]
        width *= 2
    matrix = maps_ref[chunks - 1, 0:BLOCK, :]
    diagonal = jnp.sum(jnp.where(eye, matrix, 0.0), axis=0, keepdims=True)
    tail = [p.astype(F32) for p in split3(diagonal)]
    tail += [p.astype(F32) for p in split3(maps_ref[chunks - 1, BLOCK : BLOCK + 1, :])]
    tail.append(jnp.zeros((ROWS - BLOCK - 6, BLOCK), F32))
    matrix = jnp.where(eye, 0.0, matrix).astype(BF16)
    tail = jnp.concatenate(tail, axis=0).astype(BF16)
    for peer in range(send_ref.shape[0]):
        send_ref[peer, 0:BLOCK, :] = matrix
        send_ref[peer, BLOCK:ROWS, :] = tail


def pack(index_ref, last_ref, start_ref, guess_ref, proj_ref, send_ref, row_ref, *, blocks):
    steps = guess_ref.shape[0]
    entering = jnp.where(index_ref[4] == 0, start_ref[...], last_ref[...])
    states = jnp.concatenate([entering, guess_ref[...]], axis=0)
    high = states.astype(BF16).astype(F32)
    rest = states - high
    base = (blocks + 1) * (steps + 1)
    for target in range(blocks):
        for k in range(blocks):
            row_ref[target, k * (steps + 1) : (k + 1) * (steps + 1), :] = high[
                :, k * BLOCK : (k + 1) * BLOCK
            ]
        lanes = slice(target * BLOCK, (target + 1) * BLOCK)
        row_ref[target, base - steps - 1 : base, :] = rest[:, lanes]
        for g in range(3):
            row_ref[target, base + g * steps : base + (g + 1) * steps, :] = proj_ref[
                g, :, lanes
            ].astype(F32)
        used = base + 3 * steps
        row_ref[target, used:, :] = jnp.zeros((row_ref.shape[1] - used, BLOCK), F32)
        packed = row_ref[target].astype(BF16)
        for far in range(send_ref.shape[0] // blocks):
            send_ref[far * blocks + target] = packed


def first_maps(
    index_ref, own_ref, other_ref, w_ref, ub_ref, cb_ref,
    send_ref, maps_ref, par_ref, prev_ref, guess_ref, proj_ref, row_ref,
    *, chunks, steps, blocks, stride,
):
    unit, place = index_ref[0], index_ref[1]
    states = steps + 1
    half = blocks * BLOCK
    base = (blocks + 1) * states
    length = (chunks + 1) * stride

    def rows(side, start):
        return row_ref[pl.ds(side * length + start, chunks, stride=stride), :]

    def before(side, start):
        parts = [rows(side, start + steps)]
        parts += [rows(side, stride + start + s) for s in range(1, steps)]
        return jnp.concatenate(parts, axis=0)

    total = 0.0
    for side, (ref, owner) in enumerate(((own_ref, unit), (other_ref, 1 - unit))):
        row_ref[side * length + stride : (side + 1) * length, :] = ref[...].astype(F32)
        for k in range(blocks + 1):
            row = side * length + k * states
            row_ref[row + steps : row + steps + 1, :] = row_ref[row + stride : row + stride + 1, :]
        panels = [before(side, k * states).astype(BF16) for k in range(blocks)]
        columns = w_ref[pl.ds(pl.multiple_of(owner * half, half), half), :]
        total = total + dot(jnp.concatenate(panels, axis=1), columns)
    for g in range(3):
        start = stride + base + g * steps
        proj_ref[g] = jnp.concatenate([rows(0, start + s) for s in range(steps)], axis=0)
    rest = blocks * states
    prev = before(0, place * states) + before(0, rest)
    guess = jnp.concatenate(
        [
            rows(0, stride + place * states + s + 1) + rows(0, stride + rest + s + 1)
            for s in range(steps)
        ],
        axis=0,
    )
    prev_ref[...] = prev
    guess_ref[...] = guess
    gates(total, proj_ref, prev, guess, ub_ref, cb_ref, par_ref)
    here = pl.multiple_of((unit * blocks + place) * BLOCK, BLOCK)
    compose_all(par_ref, w_ref[pl.ds(here, BLOCK), :], maps_ref, send_ref, chunks, steps)


def next_maps(
    index_ref, panel_ref, proj_ref, prev_ref, guess_ref, w_ref, ub_ref, cb_ref,
    send_ref, maps_ref, par_ref, *, chunks, steps, blocks,
):
    unit, place = index_ref[0], index_ref[1]
    sides = panel_ref.shape[0] // blocks
    panels = [panel_ref[k * sides + side] for side in range(sides) for k in range(blocks)]
    total = dot(jnp.concatenate(panels, axis=1), w_ref[...])
    gates(total, proj_ref, prev_ref[...], guess_ref[...], ub_ref, cb_ref, par_ref)
    here = pl.multiple_of((unit * blocks + place) * BLOCK, BLOCK)
    compose_all(par_ref, w_ref[pl.ds(here, BLOCK), :], maps_ref, send_ref, chunks, steps)


def solve(index_ref, got_ref, maps_ref, par_ref, w_ref, chunks, steps, blocks):
    unit, place, group = index_ref[0], index_ref[1], index_ref[2]

    def pass_group(k, delta):
        block = got_ref[k]
        matrix = block[0:BLOCK]
        tail = block[BLOCK:ROWS].astype(F32)
        diagonal = tail[0:1] + tail[1:2] + tail[2:3]
        vector = tail[3:4] + tail[4:5] + tail[5:6]
        terms = dot(
            jnp.concatenate(split2(delta), axis=1), jnp.concatenate([matrix, matrix], axis=0)
        )
        return terms + delta * diagonal + vector

    delta = lax.fori_loop(0, group, pass_group, jnp.zeros((16, BLOCK), F32))
    column = jnp.transpose(jnp.broadcast_to(delta[0:1], (BLOCK, BLOCK)))
    entries = [delta[0:1]]
    for c in range(chunks - 1):
        through = jnp.sum(column * maps_ref[c, 0:BLOCK, :], axis=0, keepdims=True)
        entries.append(through + maps_ref[c, BLOCK : BLOCK + 1, :])
    entries = jnp.concatenate(entries, axis=0)
    here = pl.multiple_of((unit * blocks + place) * BLOCK, BLOCK)
    weight = w_ref[pl.ds(here, BLOCK), :]
    double = jnp.concatenate([weight, weight], axis=0)
    current, after = entries, []
    for step in range(steps):
        current = advance_rows(current, double, par_ref, step * chunks, (step + 1) * chunks)
        after.append(current)
    return entries, after


def first_states(
    index_ref, got_ref, maps_ref, par_ref, w_ref, prev_ref, guess_ref,
    send_ref, prev_out, guess_out, *, chunks, steps, blocks,
):
    entries, after = solve(index_ref, got_ref, maps_ref, par_ref, w_ref, chunks, steps, blocks)
    prev = prev_ref[...] + jnp.concatenate([entries] + after[:-1], axis=0)
    prev_out[...] = prev
    guess_out[...] = guess_ref[...] + jnp.concatenate(after, axis=0)
    panel = prev.astype(BF16)
    for peer in range(send_ref.shape[0]):
        send_ref[peer] = panel


def last_states(
    index_ref, got_ref, maps_ref, par_ref, w_ref, guess_ref,
    send_ref, state_ref, *, chunks, steps, blocks,
):
    quarter = index_ref[3]
    _, after = solve(index_ref, got_ref, maps_ref, par_ref, w_ref, chunks, steps, blocks)
    state_ref[...] = guess_ref[...] + jnp.concatenate(after, axis=0)
    near = send_ref.shape[0]
    for peer in range(near):
        for step in range(steps):
            row = step * chunks + quarter * near + peer
            send_ref[peer, step : step + 1, :] = state_ref[pl.ds(row, 1), :]


SMEM = pl.BlockSpec(memory_space=pltpu.SMEM)
VMEM = pl.BlockSpec(memory_space=pltpu.VMEM)


def call(body, outs, args, scratch=()):
    return pl.pallas_call(
        body,
        out_shape=[jax.ShapeDtypeStruct(shape, kind) for shape, kind in outs],
        in_specs=[SMEM] + [VMEM] * (len(args) - 1),
        out_specs=[VMEM] * len(outs),
        scratch_shapes=list(scratch),
        compiler_params=pltpu.CompilerParams(vmem_limit_bytes=24 * 1024 * 1024),
        interpret=INTERPRET,
    )(*args)


def shards(projections, recurrent, update_bias, candidate_bias, start_state, initial_guess):
    _, steps, _, width_dev = projections.shape
    full_width = recurrent.shape[0]
    blocks = width_dev // BLOCK
    chunks = lax.axis_size(Z)
    near = lax.axis_size("zl")
    sides = lax.axis_size("unit")
    groups = lax.axis_size("x")
    total_steps = chunks * steps
    place = lax.axis_index("zl")
    unit = lax.axis_index("unit")
    group = lax.axis_index("x")
    time_place = lax.axis_index(TM)
    index = jnp.stack([unit, place, group, lax.axis_index("zh"), time_place]).astype(jnp.int32)

    links = [(chunks * k - 1, chunks * k) for k in range(1, groups)]
    last = lax.ppermute(initial_guess[:, -1, :], TM, links)
    weight = lax.dynamic_slice_in_dim(recurrent, place * BLOCK, BLOCK, 2)
    weight = jnp.concatenate([weight[:, g, :] for g in range(3)], axis=1)
    bias_u = lax.dynamic_slice_in_dim(update_bias, place * BLOCK, BLOCK, 0)[None]
    bias_c = lax.dynamic_slice_in_dim(candidate_bias, place * BLOCK, BLOCK, 0)[None]
    stride = -(-((blocks + 1) * (steps + 1) + 3 * steps) // 8) * 8
    (payload,) = call(
        functools.partial(pack, blocks=blocks),
        [((chunks, stride, BLOCK), BF16)],
        (index, last, start_state, initial_guess[0], jnp.transpose(projections[0], (1, 0, 2))),
        [pltpu.VMEM((blocks, stride, BLOCK), F32)],
    )
    own = lax.all_to_all(payload, Z, split_axis=0, concat_axis=0, tiled=True)
    other = lax.ppermute(own, "unit", [(s, sides - 1 - s) for s in range(sides)])
    own = own.reshape(chunks * stride, BLOCK)
    other = other.reshape(chunks * stride, BLOCK)

    sizes = dict(chunks=chunks, steps=steps, blocks=blocks)
    maps_out = [
        ((groups, ROWS, BLOCK), BF16),
        ((chunks, ROWS, BLOCK), F32),
        ((5, total_steps, BLOCK), F32),
    ]
    rows_out = [((total_steps, BLOCK), F32)] * 2
    send, maps, params, prev, guess, proj = call(
        functools.partial(first_maps, stride=stride, **sizes),
        maps_out + rows_out + [((3, total_steps, BLOCK), F32)],
        (index, own, other, weight, bias_u, bias_c),
        [pltpu.VMEM((sides * (chunks + 1) * stride, BLOCK), F32)],
    )
    got = lax.all_to_all(send, "x", split_axis=0, concat_axis=0, tiled=True)
    send, prev, guess = call(
        functools.partial(first_states, **sizes),
        [((near * sides, total_steps, BLOCK), BF16)] + rows_out,
        (index, got, maps, params, weight, prev, guess),
    )
    panels = lax.all_to_all(send, ("zl", "unit"), split_axis=0, concat_axis=0, tiled=True)
    send, maps, params = call(
        functools.partial(next_maps, **sizes),
        maps_out,
        (index, panels, proj, prev, guess, weight, bias_u, bias_c),
    )
    got = lax.all_to_all(send, "x", split_axis=0, concat_axis=0, tiled=True)
    (send,) = call(
        functools.partial(last_states, **sizes),
        [((near, steps, BLOCK), F32)],
        (index, got, maps, params, weight, guess),
        [pltpu.VMEM((total_steps, BLOCK), F32)],
    )
    final = lax.all_to_all(send, "zl", split_axis=0, concat_axis=0, tiled=True)
    return jnp.transpose(final, (1, 0, 2)).reshape(1, steps, width_dev)


def solution(mesh):
    count = mesh.shape["tm"]
    near = 4
    finer = Mesh(
        mesh.devices.reshape(
            mesh.shape["sweep"], GROUPS, count // GROUPS // near, near, mesh.shape["unit"]
        ),
        ("sweep", "x", "zh", "zl", "unit"),
    )
    return jax.shard_map(
        shards,
        mesh=finer,
        in_specs=(
            P("sweep", TM, None, "unit"),
            P("sweep", None, "unit"),
            P(("sweep", "unit")),
            P(("sweep", "unit")),
            P("sweep", "unit"),
            P("sweep", TM, "unit"),
        ),
        out_specs=P("sweep", TM, "unit"),
        check_vma=False,
    )
```

```python
import functools

import jax
import jax.numpy as jnp
from jax import lax
from jax.experimental import pallas as pl
from jax.experimental.pallas import tpu as pltpu
from jax.sharding import Mesh
from jax.sharding import PartitionSpec as P

BLOCK = 128
GROUPS = 8
TM = ("x", "zh", "zl")
Z = ("zh", "zl")
INTERPRET = False
ROWS = BLOCK + 16
F32 = jnp.float32
BF16 = jnp.bfloat16


def split2(value):
    high = value.astype(BF16)
    low = (value - high.astype(F32)).astype(BF16)
    return high, low


def split3(value):
    high = value.astype(BF16)
    rest = value - high.astype(F32)
    mid = rest.astype(BF16)
    low = (rest - mid.astype(F32)).astype(BF16)
    return high, mid, low


def dot(left, right):
    return jnp.dot(left, right, preferred_element_type=F32)


def gates(rec, proj, prev, guess, ub_ref, cb_ref, par_ref):
    update = jax.nn.sigmoid(proj[0] + rec[:, 0:BLOCK] + ub_ref[...])
    reset = jax.nn.sigmoid(proj[1] + rec[:, BLOCK : 2 * BLOCK])
    inner = rec[:, 2 * BLOCK : 3 * BLOCK] + cb_ref[...]
    cand = jnp.tanh(proj[2] + reset * inner)
    mapped = (1.0 - update) * cand + update * prev
    full = (1.0 - update) * (1.0 - cand * cand) * reset
    par_ref[0] = update
    par_ref[1] = (prev - cand) * update * (1.0 - update)
    par_ref[2] = full * inner * (1.0 - reset)
    par_ref[3] = full
    par_ref[4] = mapped - guess


def advance(value, terms, rows):
    u, a, c, d = rows
    return (
        u * value
        + a * terms[:, 0:BLOCK]
        + c * terms[:, BLOCK : 2 * BLOCK]
        + d * terms[:, 2 * BLOCK : 3 * BLOCK]
    )


def advance_rows(value, double, par_ref, low, high):
    terms = dot(jnp.concatenate(split2(value), axis=1), double)
    rows = [par_ref[i, low:high, :] for i in range(4)]
    return advance(value, terms, rows) + par_ref[4, low:high, :]


def compose_all(par_ref, weight, maps_ref, send_ref, chunks, steps, entry=None):
    eye = lax.broadcasted_iota(jnp.int32, (BLOCK, BLOCK), 0) == lax.broadcasted_iota(
        jnp.int32, (BLOCK, BLOCK), 1
    )
    wide = weight.astype(F32)
    double = jnp.concatenate([weight, weight], axis=0)
    part = 4
    for first in range(0, chunks, part):
        members = range(first, first + part)

        def rows_of(step, c):
            return [par_ref[i, step * chunks + c : step * chunks + c + 1, :] for i in range(4)]

        current = []
        for c in members:
            u, a, c_, d = rows_of(0, c)
            start = a * wide[:, 0:BLOCK] + c_ * wide[:, BLOCK : 2 * BLOCK] + d * wide[:, 2 * BLOCK :]
            current.append(start + jnp.where(eye, u, 0.0))
        for step in range(1, steps):
            stacked = jnp.concatenate([m.astype(BF16) for m in current], axis=0)
            terms = dot(stacked, weight)
            current = [
                advance(m, terms[k * BLOCK : (k + 1) * BLOCK], rows_of(step, c))
                for k, (m, c) in enumerate(zip(current, members))
            ]
        for m, c in zip(current, members):
            maps_ref[c, 0:BLOCK, :] = m
    vector = par_ref[4, 0:chunks, :]
    if entry is not None:
        vector = jnp.concatenate([entry, jnp.zeros((chunks - 1, BLOCK), F32)], axis=0)
        vector = advance_rows(vector, double, par_ref, 0, chunks)
    for step in range(1, steps):
        vector = advance_rows(vector, double, par_ref, step * chunks, (step + 1) * chunks)
    pad = jnp.zeros((ROWS - BLOCK - 1, BLOCK), F32)
    for c in range(chunks):
        maps_ref[c, BLOCK:ROWS, :] = jnp.concatenate([vector[c : c + 1], pad], axis=0)
    width = 1
    while width < chunks:
        for left in range(width - 1, chunks, 2 * width):
            before = jnp.concatenate(split2(maps_ref[left]), axis=1)
            for right in range(left + 1, left + 1 + width):
                high, low = split2(maps_ref[right, 0:BLOCK, :])
                upper = jnp.concatenate([high, low], axis=1)
                under = jnp.concatenate([high, jnp.zeros_like(low)], axis=1)
                both = dot(before, jnp.concatenate([upper, under], axis=0))
                both = both[:, 0:BLOCK] + both[:, BLOCK:]
                maps_ref[right, 0:BLOCK, :] = both[0:BLOCK]
                maps_ref[right, BLOCK:ROWS, :] = both[BLOCK:] + maps_ref[right, BLOCK:ROWS, :]
        width *= 2
    matrix = maps_ref[chunks - 1, 0:BLOCK, :]
    diagonal = jnp.sum(jnp.where(eye, matrix, 0.0), axis=0, keepdims=True)
    tail = [p.astype(F32) for p in split3(diagonal)]
    tail += [p.astype(F32) for p in split3(maps_ref[chunks - 1, BLOCK : BLOCK + 1, :])]
    tail.append(jnp.zeros((ROWS - BLOCK - 6, BLOCK), F32))
    matrix = jnp.where(eye, 0.0, matrix).astype(BF16)
    tail = jnp.concatenate(tail, axis=0).astype(BF16)
    for peer in range(send_ref.shape[0]):
        send_ref[peer, 0:BLOCK, :] = matrix
        send_ref[peer, BLOCK:ROWS, :] = tail


def pack(
    guess_hbm, proj_hbm, start_hbm, send_ref, row_ref, guess_ref, proj_ref, start_ref, sems, *, blocks
):
    copies = [
        pltpu.make_async_copy(source, target, sems.at[i])
        for i, (source, target) in enumerate(
            ((guess_hbm, guess_ref), (proj_hbm, proj_ref), (start_hbm, start_ref))
        )
    ]
    for copy in copies:
        copy.start()
    for copy in copies:
        copy.wait()
    steps = guess_ref.shape[0]
    high = guess_ref[...].astype(BF16).astype(F32)
    rest = guess_ref[...] - high
    start_high = start_ref[...].astype(BF16).astype(F32)
    start_rest = start_ref[...] - start_high
    inputs = (blocks + 1) * steps
    first = inputs + 3 * steps
    used = first + blocks + 1
    for target in range(blocks):
        lanes = slice(target * BLOCK, (target + 1) * BLOCK)
        for k in range(blocks):
            there = slice(k * BLOCK, (k + 1) * BLOCK)
            row_ref[target, k * steps : (k + 1) * steps, :] = high[:, there]
            row_ref[target, first + k : first + k + 1, :] = start_high[:, there]
        row_ref[target, blocks * steps : inputs, :] = rest[:, lanes]
        for g in range(3):
            begin = inputs + g * steps
            row_ref[target, begin : begin + steps, :] = proj_ref[g, :, lanes].astype(F32)
        row_ref[target, used - 1 : used, :] = start_rest[:, lanes]
        row_ref[target, used:, :] = jnp.zeros((row_ref.shape[1] - used, BLOCK), F32)
        packed = row_ref[target].astype(BF16)
        for far in range(send_ref.shape[0] // blocks):
            send_ref[far * blocks + target] = packed


def first_maps(
    index_ref, own_ref, other_ref, next_ref, w_ref, ub_ref, cb_ref,
    send_ref, maps_ref, par_ref, prev_ref, guess_ref, proj_ref, row_ref,
    *, chunks, steps, blocks, stride,
):
    unit, place, group = index_ref[0], index_ref[1], index_ref[2]
    half = blocks * BLOCK
    inputs = (blocks + 1) * steps
    first = inputs + 3 * steps
    length = (chunks + 1) * stride
    total_steps = chunks * steps
    extra = 16

    def rows(side, start):
        return row_ref[pl.ds(side * length + start, chunks, stride=stride), :]

    def all_steps(side, start):
        return [rows(side, start + s) for s in range(steps)]

    def later(start):
        return [rows(0, start + s) for s in range(1, steps)] + [rows(0, stride + start)]

    def one(start, side=0):
        row = row_ref[pl.ds(side * length + start, 1), :]
        return jnp.broadcast_to(row, (extra, BLOCK))

    row_ref[length - stride : length, :] = next_ref[...].astype(F32)
    total = 0.0
    for side, (ref, owner) in enumerate(((own_ref, unit), (other_ref, 1 - unit))):
        row_ref[side * length : side * length + chunks * stride, :] = ref[...].astype(F32)
        panels = [
            jnp.concatenate(all_steps(side, k * steps) + [one(first + k, side)], axis=0).astype(BF16)
            for k in range(blocks)
        ]
        columns = w_ref[pl.ds(pl.multiple_of(owner * half, half), half), :]
        total = total + dot(jnp.concatenate(panels, axis=1), columns)
    proj = []
    for g in range(3):
        start = inputs + g * steps
        proj.append(jnp.concatenate(later(start) + [one(start)], axis=0))
        proj_ref[g] = proj[g][0:total_steps]
    own, rest = place * steps, blocks * steps
    begin = one(first + place) + one(first + blocks)
    prev = jnp.concatenate(all_steps(0, own) + [begin], axis=0)
    prev += jnp.concatenate(all_steps(0, rest) + [jnp.zeros_like(begin)], axis=0)
    guess = jnp.concatenate(later(own) + [one(own)], axis=0)
    guess += jnp.concatenate(later(rest) + [one(rest)], axis=0)
    prev_ref[...] = prev[0:total_steps]
    guess_ref[...] = guess[0:total_steps]
    gates(total, proj, prev, guess, ub_ref, cb_ref, par_ref)
    entry = jnp.where(group == 0, par_ref[4, total_steps : total_steps + 1, :], 0.0)
    par_ref[4, total_steps : total_steps + 1, :] = entry
    here = pl.multiple_of((unit * blocks + place) * BLOCK, BLOCK)
    compose_all(par_ref, w_ref[pl.ds(here, BLOCK), :], maps_ref, send_ref, chunks, steps, entry)


def next_maps(
    index_ref, panel_ref, proj_ref, prev_ref, guess_ref, w_ref, ub_ref, cb_ref,
    send_ref, maps_ref, par_ref, *, chunks, steps, blocks,
):
    unit, place = index_ref[0], index_ref[1]
    sides = panel_ref.shape[0] // blocks
    panels = [panel_ref[k * sides + side] for side in range(sides) for k in range(blocks)]
    total = dot(jnp.concatenate(panels, axis=1), w_ref[...])
    gates(total, proj_ref, prev_ref[...], guess_ref[...], ub_ref, cb_ref, par_ref)
    here = pl.multiple_of((unit * blocks + place) * BLOCK, BLOCK)
    compose_all(par_ref, w_ref[pl.ds(here, BLOCK), :], maps_ref, send_ref, chunks, steps)


def solve(index_ref, got_ref, maps_ref, par_ref, w_ref, chunks, steps, blocks, entry=0.0):
    unit, place, group = index_ref[0], index_ref[1], index_ref[2]

    def pass_group(k, delta):
        block = got_ref[k]
        matrix = block[0:BLOCK]
        tail = block[BLOCK:ROWS].astype(F32)
        diagonal = tail[0:1] + tail[1:2] + tail[2:3]
        vector = tail[3:4] + tail[4:5] + tail[5:6]
        terms = dot(
            jnp.concatenate(split2(delta), axis=1), jnp.concatenate([matrix, matrix], axis=0)
        )
        return terms + delta * diagonal + vector

    delta = lax.fori_loop(0, group, pass_group, jnp.zeros((16, BLOCK), F32))
    column = jnp.transpose(jnp.broadcast_to(delta[0:1], (BLOCK, BLOCK)))
    entries = [delta[0:1] + entry]
    for c in range(chunks - 1):
        through = jnp.sum(column * maps_ref[c, 0:BLOCK, :], axis=0, keepdims=True)
        entries.append(through + maps_ref[c, BLOCK : BLOCK + 1, :])
    entries = jnp.concatenate(entries, axis=0)
    here = pl.multiple_of((unit * blocks + place) * BLOCK, BLOCK)
    weight = w_ref[pl.ds(here, BLOCK), :]
    double = jnp.concatenate([weight, weight], axis=0)
    current, after = entries, []
    for step in range(steps):
        current = advance_rows(current, double, par_ref, step * chunks, (step + 1) * chunks)
        after.append(current)
    return entries, after


def first_states(
    index_ref, got_ref, maps_ref, par_ref, w_ref, prev_ref, guess_ref,
    send_ref, prev_out, guess_out, *, chunks, steps, blocks,
):
    entry = par_ref[4, chunks * steps : chunks * steps + 1, :]
    entries, after = solve(
        index_ref, got_ref, maps_ref, par_ref, w_ref, chunks, steps, blocks, entry
    )
    prev = prev_ref[...] + jnp.concatenate([entries] + after[:-1], axis=0)
    prev_out[...] = prev
    guess_out[...] = guess_ref[...] + jnp.concatenate(after, axis=0)
    panel = prev.astype(BF16)
    for peer in range(send_ref.shape[0]):
        send_ref[peer] = panel


def last_states(
    index_ref, got_ref, maps_ref, par_ref, w_ref, prev_ref,
    send_ref, state_ref, *, chunks, steps, blocks,
):
    quarter = index_ref[3]
    entries, after = solve(index_ref, got_ref, maps_ref, par_ref, w_ref, chunks, steps - 1, blocks)
    state_ref[...] = prev_ref[...] + jnp.concatenate([entries] + after, axis=0)
    near = send_ref.shape[0]
    for peer in range(near):
        for step in range(steps):
            row = step * chunks + quarter * near + peer
            send_ref[peer, step : step + 1, :] = state_ref[pl.ds(row, 1), :]


SMEM = pl.BlockSpec(memory_space=pltpu.SMEM)
VMEM = pl.BlockSpec(memory_space=pltpu.VMEM)


def call(body, outs, args, scratch=(), first=SMEM, rest=VMEM, limit=24 * 1024 * 1024):
    return pl.pallas_call(
        body,
        out_shape=[jax.ShapeDtypeStruct(shape, kind) for shape, kind in outs],
        in_specs=[first] + [rest] * (len(args) - 1),
        out_specs=[VMEM] * len(outs),
        scratch_shapes=list(scratch),
        compiler_params=pltpu.CompilerParams(vmem_limit_bytes=limit),
        interpret=INTERPRET,
    )(*args)


def shards(projections, recurrent, update_bias, candidate_bias, start_state, initial_guess):
    _, steps, _, width_dev = projections.shape
    full_width = recurrent.shape[0]
    blocks = width_dev // BLOCK
    chunks = lax.axis_size(Z)
    near = lax.axis_size("zl")
    sides = lax.axis_size("unit")
    groups = lax.axis_size("x")
    total_steps = chunks * steps
    place = lax.axis_index("zl")
    unit = lax.axis_index("unit")
    group = lax.axis_index("x")
    index = jnp.stack([unit, place, group, lax.axis_index("zh")]).astype(jnp.int32)

    weight = lax.dynamic_slice_in_dim(recurrent, place * BLOCK, BLOCK, 2)
    weight = jnp.concatenate([weight[:, g, :] for g in range(3)], axis=1)
    bias_u = lax.dynamic_slice_in_dim(update_bias, place * BLOCK, BLOCK, 0)[None]
    bias_c = lax.dynamic_slice_in_dim(candidate_bias, place * BLOCK, BLOCK, 0)[None]
    stride = -(-((blocks + 1) * (steps + 1) + 3 * steps) // 8) * 8
    here = pl.BlockSpec(memory_space=pl.ANY)
    (payload,) = call(
        functools.partial(pack, blocks=blocks),
        [((chunks, stride, BLOCK), BF16)],
        (initial_guess[0], jnp.transpose(projections[0], (1, 0, 2)), start_state),
        [
            pltpu.VMEM((blocks, stride, BLOCK), F32),
            pltpu.VMEM((steps, width_dev), F32),
            pltpu.VMEM((3, steps, width_dev), BF16),
            pltpu.VMEM((1, width_dev), F32),
            pltpu.SemaphoreType.DMA((3,)),
        ],
        here,
        here,
        60 * 1024 * 1024,
    )
    own = lax.all_to_all(payload, Z, split_axis=0, concat_axis=0, tiled=True)
    after = lax.ppermute(own[0], "x", [(k + 1, k) for k in range(groups - 1)])
    other = lax.ppermute(own, "unit", [(s, sides - 1 - s) for s in range(sides)])
    own = own.reshape(chunks * stride, BLOCK)
    other = other.reshape(chunks * stride, BLOCK)

    sizes = dict(chunks=chunks, steps=steps, blocks=blocks)
    maps_out = [
        ((groups, ROWS, BLOCK), BF16),
        ((chunks, ROWS, BLOCK), F32),
        ((5, total_steps, BLOCK), F32),
    ]
    rows_out = [((total_steps, BLOCK), F32)] * 2
    first_out = maps_out[:2] + [((5, total_steps + 16, BLOCK), F32)]
    send, maps, params, prev, guess, proj = call(
        functools.partial(first_maps, stride=stride, **sizes),
        first_out + rows_out + [((3, total_steps, BLOCK), F32)],
        (index, own, other, after, weight, bias_u, bias_c),
        [pltpu.VMEM((sides * (chunks + 1) * stride, BLOCK), F32)],
    )
    got = lax.all_to_all(send, "x", split_axis=0, concat_axis=0, tiled=True)
    send, prev, guess = call(
        functools.partial(first_states, **sizes),
        [((near * sides, total_steps, BLOCK), BF16)] + rows_out,
        (index, got, maps, params, weight, prev, guess),
    )
    panels = lax.all_to_all(send, ("zl", "unit"), split_axis=0, concat_axis=0, tiled=True)
    send, maps, params = call(
        functools.partial(next_maps, **sizes),
        maps_out,
        (index, panels, proj, prev, guess, weight, bias_u, bias_c),
    )
    got = lax.all_to_all(send, "x", split_axis=0, concat_axis=0, tiled=True)
    (send,) = call(
        functools.partial(last_states, **sizes),
        [((near, steps, BLOCK), F32)],
        (index, got, maps, params, weight, prev),
        [pltpu.VMEM((total_steps, BLOCK), F32)],
    )
    final = lax.all_to_all(send, "zl", split_axis=0, concat_axis=0, tiled=True)
    return jnp.transpose(final, (1, 0, 2)).reshape(1, steps, width_dev)


def solution(mesh):
    count = mesh.shape["tm"]
    near = 4
    finer = Mesh(
        mesh.devices.reshape(
            mesh.shape["sweep"], GROUPS, count // GROUPS // near, near, mesh.shape["unit"]
        ),
        ("sweep", "x", "zh", "zl", "unit"),
    )
    return jax.shard_map(
        shards,
        mesh=finer,
        in_specs=(
            P("sweep", TM, None, "unit"),
            P("sweep", None, "unit"),
            P(("sweep", "unit")),
            P(("sweep", "unit")),
            P("sweep", "unit"),
            P("sweep", TM, "unit"),
        ),
        out_specs=P("sweep", TM, "unit"),
        check_vma=False,
    )
```

```python
import functools

import jax
import jax.numpy as jnp
from jax import lax
from jax.experimental import pallas as pl
from jax.experimental.pallas import tpu as pltpu
from jax.sharding import Mesh
from jax.sharding import PartitionSpec as P

BLOCK = 128
GROUPS = 8
TM = ("x", "zh", "zl")
Z = ("zh", "zl")
INTERPRET = False
ROWS = BLOCK + 16
F32 = jnp.float32
BF16 = jnp.bfloat16


def split2(value):
    high = value.astype(BF16)
    low = (value - high.astype(F32)).astype(BF16)
    return high, low


def split3(value):
    high = value.astype(BF16)
    rest = value - high.astype(F32)
    mid = rest.astype(BF16)
    low = (rest - mid.astype(F32)).astype(BF16)
    return high, mid, low


def dot(left, right):
    return jnp.dot(left, right, preferred_element_type=F32)


def gates(rec, proj, prev, guess, ub_ref, cb_ref, par_ref, low=0):
    update = jax.nn.sigmoid(proj[0] + rec[:, 0:BLOCK] + ub_ref[...])
    reset = jax.nn.sigmoid(proj[1] + rec[:, BLOCK : 2 * BLOCK])
    inner = rec[:, 2 * BLOCK : 3 * BLOCK] + cb_ref[...]
    cand = jnp.tanh(proj[2] + reset * inner)
    mapped = (1.0 - update) * cand + update * prev
    full = (1.0 - update) * (1.0 - cand * cand) * reset
    high = low + rec.shape[0]
    par_ref[0, low:high] = update
    par_ref[1, low:high] = (prev - cand) * update * (1.0 - update)
    par_ref[2, low:high] = full * inner * (1.0 - reset)
    par_ref[3, low:high] = full
    par_ref[4, low:high] = mapped - guess


def advance(value, terms, rows):
    u, a, c, d = rows
    return (
        u * value
        + a * terms[:, 0:BLOCK]
        + c * terms[:, BLOCK : 2 * BLOCK]
        + d * terms[:, 2 * BLOCK : 3 * BLOCK]
    )


def advance_rows(value, double, par_ref, low, high):
    terms = dot(jnp.concatenate(split2(value), axis=1), double)
    rows = [par_ref[i, low:high, :] for i in range(4)]
    return advance(value, terms, rows) + par_ref[4, low:high, :]


PART = 4


def diagonal_mask():
    shape = (BLOCK, BLOCK)
    return lax.broadcasted_iota(jnp.int32, shape, 0) == lax.broadcasted_iota(jnp.int32, shape, 1)


def compose_chunks(par_ref, weight, maps_ref, begin, end, chunks, steps):
    eye = diagonal_mask()
    wide = weight.astype(F32)
    for first in range(begin, end, PART):
        members = range(first, first + PART)

        def rows_of(step, c):
            return [par_ref[i, step * chunks + c : step * chunks + c + 1, :] for i in range(4)]

        current = []
        for c in members:
            u, a, c_, d = rows_of(0, c)
            start = a * wide[:, 0:BLOCK] + c_ * wide[:, BLOCK : 2 * BLOCK] + d * wide[:, 2 * BLOCK :]
            current.append(start + jnp.where(eye, u, 0.0))
        for step in range(1, steps):
            stacked = jnp.concatenate([m.astype(BF16) for m in current], axis=0)
            terms = dot(stacked, weight)
            current = [
                advance(m, terms[k * BLOCK : (k + 1) * BLOCK], rows_of(step, c))
                for k, (m, c) in enumerate(zip(current, members))
            ]
        for m, c in zip(current, members):
            maps_ref[c, 0:BLOCK, :] = m


def scan_chunks(par_ref, weight, maps_ref, send_ref, chunks, steps, entry=None):
    eye = diagonal_mask()
    double = jnp.concatenate([weight, weight], axis=0)
    vector = par_ref[4, 0:chunks, :]
    if entry is not None:
        vector = jnp.concatenate([entry, jnp.zeros((chunks - 1, BLOCK), F32)], axis=0)
        vector = advance_rows(vector, double, par_ref, 0, chunks)
    for step in range(1, steps):
        vector = advance_rows(vector, double, par_ref, step * chunks, (step + 1) * chunks)
    pad = jnp.zeros((ROWS - BLOCK - 1, BLOCK), F32)
    for c in range(chunks):
        maps_ref[c, BLOCK:ROWS, :] = jnp.concatenate([vector[c : c + 1], pad], axis=0)
    width = 1
    while width < chunks:
        for left in range(width - 1, chunks, 2 * width):
            before = jnp.concatenate(split2(maps_ref[left]), axis=1)
            for right in range(left + 1, left + 1 + width):
                high, low = split2(maps_ref[right, 0:BLOCK, :])
                upper = jnp.concatenate([high, low], axis=1)
                under = jnp.concatenate([high, jnp.zeros_like(low)], axis=1)
                both = dot(before, jnp.concatenate([upper, under], axis=0))
                both = both[:, 0:BLOCK] + both[:, BLOCK:]
                maps_ref[right, 0:BLOCK, :] = both[0:BLOCK]
                maps_ref[right, BLOCK:ROWS, :] = both[BLOCK:] + maps_ref[right, BLOCK:ROWS, :]
        width *= 2
    matrix = maps_ref[chunks - 1, 0:BLOCK, :]
    diagonal = jnp.sum(jnp.where(eye, matrix, 0.0), axis=0, keepdims=True)
    tail = [p.astype(F32) for p in split3(diagonal)]
    tail += [p.astype(F32) for p in split3(maps_ref[chunks - 1, BLOCK : BLOCK + 1, :])]
    tail.append(jnp.zeros((ROWS - BLOCK - 6, BLOCK), F32))
    matrix = jnp.where(eye, 0.0, matrix).astype(BF16)
    tail = jnp.concatenate(tail, axis=0).astype(BF16)
    for peer in range(send_ref.shape[0]):
        send_ref[peer, 0:BLOCK, :] = matrix
        send_ref[peer, BLOCK:ROWS, :] = tail


def pack(
    guess_hbm, proj_hbm, start_hbm, send_ref, row_ref, guess_ref, proj_ref, start_ref, sems, *, blocks
):
    copies = [
        pltpu.make_async_copy(source, target, sems.at[i])
        for i, (source, target) in enumerate(
            ((guess_hbm, guess_ref), (proj_hbm, proj_ref), (start_hbm, start_ref))
        )
    ]
    for copy in copies:
        copy.start()
    for copy in copies:
        copy.wait()
    steps = guess_ref.shape[0]
    high = guess_ref[...].astype(BF16).astype(F32)
    rest = guess_ref[...] - high
    start_high = start_ref[...].astype(BF16).astype(F32)
    start_rest = start_ref[...] - start_high
    inputs = (blocks + 1) * steps
    first = inputs + 3 * steps
    used = first + blocks + 1
    for target in range(blocks):
        lanes = slice(target * BLOCK, (target + 1) * BLOCK)
        for k in range(blocks):
            there = slice(k * BLOCK, (k + 1) * BLOCK)
            row_ref[target, k * steps : (k + 1) * steps, :] = high[:, there]
            row_ref[target, first + k : first + k + 1, :] = start_high[:, there]
        row_ref[target, blocks * steps : inputs, :] = rest[:, lanes]
        for g in range(3):
            begin = inputs + g * steps
            row_ref[target, begin : begin + steps, :] = proj_ref[g, :, lanes].astype(F32)
        row_ref[target, used - 1 : used, :] = start_rest[:, lanes]
        row_ref[target, used:, :] = jnp.zeros((row_ref.shape[1] - used, BLOCK), F32)
        packed = row_ref[target].astype(BF16)
        for far in range(send_ref.shape[0] // blocks):
            send_ref[far * blocks + target] = packed


def first_maps(
    index_ref, own_ref, other_ref, w_ref, ub_ref, cb_ref,
    maps_ref, par_ref, prev_ref, guess_ref, proj_ref, rec_ref, row_ref,
    *, chunks, steps, blocks, stride,
):
    unit, place, group = index_ref[0], index_ref[1], index_ref[2]
    half = blocks * BLOCK
    inputs = (blocks + 1) * steps
    first = inputs + 3 * steps
    length = (chunks + 1) * stride
    total_steps = chunks * steps
    extra = 16

    def rows(side, start):
        return row_ref[pl.ds(side * length + start, chunks, stride=stride), :]

    def all_steps(side, start):
        return [rows(side, start + s) for s in range(steps)]

    def later(start):
        return [rows(0, start + s) for s in range(1, steps)] + [rows(0, stride + start)]

    def one(start, side=0):
        row = row_ref[pl.ds(side * length + start, 1), :]
        return jnp.broadcast_to(row, (extra, BLOCK))

    row_ref[length - stride : length, :] = jnp.zeros((stride, BLOCK), F32)
    total = 0.0
    for side, (ref, owner) in enumerate(((own_ref, unit), (other_ref, 1 - unit))):
        row_ref[side * length : side * length + chunks * stride, :] = ref[...].astype(F32)
        panels = [
            jnp.concatenate(all_steps(side, k * steps) + [one(first + k, side)], axis=0).astype(BF16)
            for k in range(blocks)
        ]
        columns = w_ref[pl.ds(pl.multiple_of(owner * half, half), half), :]
        total = total + dot(jnp.concatenate(panels, axis=1), columns)
    proj = []
    for g in range(3):
        start = inputs + g * steps
        proj.append(jnp.concatenate(later(start) + [one(start)], axis=0))
        proj_ref[g] = proj[g][0:total_steps]
    own, rest = place * steps, blocks * steps
    begin = one(first + place) + one(first + blocks)
    prev = jnp.concatenate(all_steps(0, own) + [begin], axis=0)
    prev += jnp.concatenate(all_steps(0, rest) + [jnp.zeros_like(begin)], axis=0)
    guess = jnp.concatenate(later(own) + [one(own)], axis=0)
    guess += jnp.concatenate(later(rest) + [one(rest)], axis=0)
    prev_ref[...] = prev[0:total_steps]
    guess_ref[...] = guess[0:total_steps]
    gates(total, proj, prev, guess, ub_ref, cb_ref, par_ref)
    entry = jnp.where(group == 0, par_ref[4, total_steps : total_steps + 1, :], 0.0)
    par_ref[4, total_steps : total_steps + 1, :] = entry
    rec_ref[...] = total[total_steps - chunks : total_steps]
    here = pl.multiple_of((unit * blocks + place) * BLOCK, BLOCK)
    weight = w_ref[pl.ds(here, BLOCK), :]
    compose_chunks(par_ref, weight, maps_ref, 0, maps_ref.shape[0], chunks, steps)


def finish_maps(
    index_ref, next_ref, rec_ref, w_ref, ub_ref, cb_ref, some_ref, par_in, prev_ref, guess_in, proj_in,
    send_ref, maps_ref, par_ref, guess_ref, proj_ref, row_ref,
    *, chunks, steps, blocks,
):
    unit, place = index_ref[0], index_ref[1]
    total_steps = chunks * steps
    low = total_steps - chunks
    done = some_ref.shape[0]
    inputs = (blocks + 1) * steps
    row_ref[...] = next_ref[...].astype(F32)
    last = lax.broadcasted_iota(jnp.int32, (chunks, BLOCK), 0) == chunks - 1

    def row(start):
        return row_ref[pl.ds(start, 1), :]

    par_ref[...] = par_in[...]
    guess_ref[...] = guess_in[...]
    proj_ref[...] = proj_in[...]
    proj = []
    for g in range(3):
        proj.append(jnp.where(last, row(inputs + g * steps), proj_in[g, low:total_steps, :]))
        proj_ref[g, low:total_steps, :] = proj[g]
    guess = row(place * steps) + row(blocks * steps)
    guess = jnp.where(last, guess, guess_in[low:total_steps, :])
    guess_ref[low:total_steps, :] = guess
    prev = prev_ref[low:total_steps, :]
    gates(rec_ref[...], proj, prev, guess, ub_ref, cb_ref, par_ref, low)
    here = pl.multiple_of((unit * blocks + place) * BLOCK, BLOCK)
    weight = w_ref[pl.ds(here, BLOCK), :]
    compose_chunks(par_ref, weight, maps_ref, done, chunks, chunks, steps)
    for c in range(done):
        maps_ref[c, 0:BLOCK, :] = some_ref[c]
    entry = par_in[4, total_steps : total_steps + 1, :]
    scan_chunks(par_ref, weight, maps_ref, send_ref, chunks, steps, entry)


def next_maps(
    index_ref, panel_ref, proj_ref, prev_ref, guess_ref, w_ref, ub_ref, cb_ref,
    send_ref, maps_ref, par_ref, *, chunks, steps, blocks,
):
    unit, place = index_ref[0], index_ref[1]
    sides = panel_ref.shape[0] // blocks
    panels = [panel_ref[k * sides + side] for side in range(sides) for k in range(blocks)]
    total = dot(jnp.concatenate(panels, axis=1), w_ref[...])
    gates(total, proj_ref, prev_ref[...], guess_ref[...], ub_ref, cb_ref, par_ref)
    here = pl.multiple_of((unit * blocks + place) * BLOCK, BLOCK)
    weight = w_ref[pl.ds(here, BLOCK), :]
    compose_chunks(par_ref, weight, maps_ref, 0, chunks, chunks, steps)
    scan_chunks(par_ref, weight, maps_ref, send_ref, chunks, steps)


def solve(index_ref, got_ref, maps_ref, par_ref, w_ref, chunks, steps, blocks, entry=0.0):
    unit, place, group = index_ref[0], index_ref[1], index_ref[2]

    def pass_group(k, delta):
        block = got_ref[k]
        matrix = block[0:BLOCK]
        tail = block[BLOCK:ROWS].astype(F32)
        diagonal = tail[0:1] + tail[1:2] + tail[2:3]
        vector = tail[3:4] + tail[4:5] + tail[5:6]
        terms = dot(
            jnp.concatenate(split2(delta), axis=1), jnp.concatenate([matrix, matrix], axis=0)
        )
        return terms + delta * diagonal + vector

    delta = lax.fori_loop(0, group, pass_group, jnp.zeros((16, BLOCK), F32))
    column = jnp.transpose(jnp.broadcast_to(delta[0:1], (BLOCK, BLOCK)))
    entries = [delta[0:1] + entry]
    for c in range(chunks - 1):
        through = jnp.sum(column * maps_ref[c, 0:BLOCK, :], axis=0, keepdims=True)
        entries.append(through + maps_ref[c, BLOCK : BLOCK + 1, :])
    entries = jnp.concatenate(entries, axis=0)
    here = pl.multiple_of((unit * blocks + place) * BLOCK, BLOCK)
    weight = w_ref[pl.ds(here, BLOCK), :]
    double = jnp.concatenate([weight, weight], axis=0)
    current, after = entries, []
    for step in range(steps):
        current = advance_rows(current, double, par_ref, step * chunks, (step + 1) * chunks)
        after.append(current)
    return entries, after


def first_states(
    index_ref, got_ref, maps_ref, par_ref, w_ref, prev_ref, guess_ref,
    send_ref, prev_out, guess_out, *, chunks, steps, blocks,
):
    entry = par_ref[4, chunks * steps : chunks * steps + 1, :]
    entries, after = solve(
        index_ref, got_ref, maps_ref, par_ref, w_ref, chunks, steps, blocks, entry
    )
    prev = prev_ref[...] + jnp.concatenate([entries] + after[:-1], axis=0)
    prev_out[...] = prev
    guess_out[...] = guess_ref[...] + jnp.concatenate(after, axis=0)
    panel = prev.astype(BF16)
    for peer in range(send_ref.shape[0]):
        send_ref[peer] = panel


def last_states(
    index_ref, got_ref, maps_ref, par_ref, w_ref, prev_ref,
    send_ref, state_ref, *, chunks, steps, blocks,
):
    quarter = index_ref[3]
    entries, after = solve(index_ref, got_ref, maps_ref, par_ref, w_ref, chunks, steps - 1, blocks)
    state_ref[...] = prev_ref[...] + jnp.concatenate([entries] + after, axis=0)
    near = send_ref.shape[0]
    for peer in range(near):
        for step in range(steps):
            row = step * chunks + quarter * near + peer
            send_ref[peer, step : step + 1, :] = state_ref[pl.ds(row, 1), :]


SMEM = pl.BlockSpec(memory_space=pltpu.SMEM)
VMEM = pl.BlockSpec(memory_space=pltpu.VMEM)


def call(
    body, outs, args, scratch=(), first=SMEM, rest=VMEM, limit=24 * 1024 * 1024, cost=None
):
    return pl.pallas_call(
        body,
        out_shape=[jax.ShapeDtypeStruct(shape, kind) for shape, kind in outs],
        in_specs=[first] + [rest] * (len(args) - 1),
        out_specs=[VMEM] * len(outs),
        scratch_shapes=list(scratch),
        compiler_params=pltpu.CompilerParams(vmem_limit_bytes=limit),
        cost_estimate=cost,
        interpret=INTERPRET,
    )(*args)


def shards(projections, recurrent, update_bias, candidate_bias, start_state, initial_guess):
    _, steps, _, width_dev = projections.shape
    full_width = recurrent.shape[0]
    blocks = width_dev // BLOCK
    chunks = lax.axis_size(Z)
    near = lax.axis_size("zl")
    sides = lax.axis_size("unit")
    groups = lax.axis_size("x")
    total_steps = chunks * steps
    place = lax.axis_index("zl")
    unit = lax.axis_index("unit")
    group = lax.axis_index("x")
    index = jnp.stack([unit, place, group, lax.axis_index("zh")]).astype(jnp.int32)

    weight = lax.dynamic_slice_in_dim(recurrent, place * BLOCK, BLOCK, 2)
    weight = jnp.concatenate([weight[:, g, :] for g in range(3)], axis=1)
    bias_u = lax.dynamic_slice_in_dim(update_bias, place * BLOCK, BLOCK, 0)[None]
    bias_c = lax.dynamic_slice_in_dim(candidate_bias, place * BLOCK, BLOCK, 0)[None]
    stride = -(-((blocks + 1) * (steps + 1) + 3 * steps) // 8) * 8
    here = pl.BlockSpec(memory_space=pl.ANY)
    (payload,) = call(
        functools.partial(pack, blocks=blocks),
        [((chunks, stride, BLOCK), BF16)],
        (initial_guess[0], jnp.transpose(projections[0], (1, 0, 2)), start_state),
        [
            pltpu.VMEM((blocks, stride, BLOCK), F32),
            pltpu.VMEM((steps, width_dev), F32),
            pltpu.VMEM((3, steps, width_dev), BF16),
            pltpu.VMEM((1, width_dev), F32),
            pltpu.SemaphoreType.DMA((3,)),
        ],
        here,
        here,
        60 * 1024 * 1024,
    )
    own = lax.all_to_all(payload, Z, split_axis=0, concat_axis=0, tiled=True)
    after = lax.ppermute(own[0], "x", [(k + 1, k) for k in range(groups - 1)])
    other = lax.ppermute(own, "unit", [(s, sides - 1 - s) for s in range(sides)])
    own = own.reshape(chunks * stride, BLOCK)
    other = other.reshape(chunks * stride, BLOCK)

    sizes = dict(chunks=chunks, steps=steps, blocks=blocks)
    maps_out = [
        ((groups, ROWS, BLOCK), BF16),
        ((chunks, ROWS, BLOCK), F32),
        ((5, total_steps, BLOCK), F32),
    ]
    rows_out = [((total_steps, BLOCK), F32)] * 2
    params_out = [((5, total_steps + 16, BLOCK), F32)]
    proj_out = [((3, total_steps, BLOCK), F32)]
    some, params, prev, guess, proj, rec = call(
        functools.partial(first_maps, stride=stride, **sizes),
        [((chunks - PART, BLOCK, BLOCK), F32)]
        + params_out
        + rows_out
        + proj_out
        + [((chunks, 3 * BLOCK), F32)],
        (index, own, other, weight, bias_u, bias_c),
        [pltpu.VMEM((sides * (chunks + 1) * stride, BLOCK), F32)],
        cost=pl.CostEstimate(flops=4 * 10**9, bytes_accessed=4 * 10**6, transcendentals=0),
    )
    send, maps, params, guess, proj = call(
        functools.partial(finish_maps, **sizes),
        maps_out[:2] + params_out + rows_out[:1] + proj_out,
        (index, after, rec, weight, bias_u, bias_c, some, params, prev, guess, proj),
        [pltpu.VMEM((stride, BLOCK), F32)],
    )
    got = lax.all_to_all(send, "x", split_axis=0, concat_axis=0, tiled=True)
    send, prev, guess = call(
        functools.partial(first_states, **sizes),
        [((near * sides, total_steps, BLOCK), BF16)] + rows_out,
        (index, got, maps, params, weight, prev, guess),
    )
    panels = lax.all_to_all(send, ("zl", "unit"), split_axis=0, concat_axis=0, tiled=True)
    send, maps, params = call(
        functools.partial(next_maps, **sizes),
        maps_out,
        (index, panels, proj, prev, guess, weight, bias_u, bias_c),
    )
    got = lax.all_to_all(send, "x", split_axis=0, concat_axis=0, tiled=True)
    (send,) = call(
        functools.partial(last_states, **sizes),
        [((near, steps, BLOCK), F32)],
        (index, got, maps, params, weight, prev),
        [pltpu.VMEM((total_steps, BLOCK), F32)],
    )
    final = lax.all_to_all(send, "zl", split_axis=0, concat_axis=0, tiled=True)
    return jnp.transpose(final, (1, 0, 2)).reshape(1, steps, width_dev)


def solution(mesh):
    count = mesh.shape["tm"]
    near = 4
    finer = Mesh(
        mesh.devices.reshape(
            mesh.shape["sweep"], GROUPS, count // GROUPS // near, near, mesh.shape["unit"]
        ),
        ("sweep", "x", "zh", "zl", "unit"),
    )
    return jax.shard_map(
        shards,
        mesh=finer,
        in_specs=(
            P("sweep", TM, None, "unit"),
            P("sweep", None, "unit"),
            P(("sweep", "unit")),
            P(("sweep", "unit")),
            P("sweep", "unit"),
            P("sweep", TM, "unit"),
        ),
        out_specs=P("sweep", TM, "unit"),
        check_vma=False,
    )
```

```python
import functools

import jax
import jax.numpy as jnp
from jax import lax
from jax.experimental import pallas as pl
from jax.experimental.pallas import tpu as pltpu
from jax.sharding import Mesh
from jax.sharding import PartitionSpec as P

BLOCK = 128
GROUPS = 8
TM = ("x", "zh", "zl")
Z = ("zh", "zl")
INTERPRET = False
ROWS = BLOCK + 16
F32 = jnp.float32
BF16 = jnp.bfloat16


def split2(value):
    high = value.astype(BF16)
    low = (value - high.astype(F32)).astype(BF16)
    return high, low


def split3(value):
    high = value.astype(BF16)
    rest = value - high.astype(F32)
    mid = rest.astype(BF16)
    low = (rest - mid.astype(F32)).astype(BF16)
    return high, mid, low


def dot(left, right):
    return jnp.dot(left, right, preferred_element_type=F32)


def columns(w_ref, begin, count):
    begin = pl.multiple_of(begin, BLOCK)
    return jnp.concatenate([w_ref[g, pl.ds(begin, count), :] for g in range(3)], axis=1)


def gates(rec, proj, prev, guess, ub_ref, cb_ref, par_ref, low=0):
    update = jax.nn.sigmoid(proj[0] + rec[:, 0:BLOCK] + ub_ref[...])
    reset = jax.nn.sigmoid(proj[1] + rec[:, BLOCK : 2 * BLOCK])
    inner = rec[:, 2 * BLOCK : 3 * BLOCK] + cb_ref[...]
    cand = jnp.tanh(proj[2] + reset * inner)
    mapped = (1.0 - update) * cand + update * prev
    full = (1.0 - update) * (1.0 - cand * cand) * reset
    high = low + rec.shape[0]
    par_ref[0, low:high] = update
    par_ref[1, low:high] = (prev - cand) * update * (1.0 - update)
    par_ref[2, low:high] = full * inner * (1.0 - reset)
    par_ref[3, low:high] = full
    par_ref[4, low:high] = mapped - guess


def advance(value, terms, rows):
    u, a, c, d = rows
    return (
        u * value
        + a * terms[:, 0:BLOCK]
        + c * terms[:, BLOCK : 2 * BLOCK]
        + d * terms[:, 2 * BLOCK : 3 * BLOCK]
    )


def advance_rows(value, double, par_ref, low, high):
    terms = dot(jnp.concatenate(split2(value), axis=1), double)
    rows = [par_ref[i, low:high, :] for i in range(4)]
    return advance(value, terms, rows) + par_ref[4, low:high, :]


PART = 4


def diagonal_mask():
    shape = (BLOCK, BLOCK)
    return lax.broadcasted_iota(jnp.int32, shape, 0) == lax.broadcasted_iota(jnp.int32, shape, 1)


def compose_chunks(par_ref, weight, maps_ref, begin, end, chunks, steps):
    eye = diagonal_mask()
    wide = weight.astype(F32)
    for first in range(begin, end, PART):
        members = range(first, first + PART)

        def rows_of(step, c):
            return [par_ref[i, step * chunks + c : step * chunks + c + 1, :] for i in range(4)]

        current = []
        for c in members:
            u, a, c_, d = rows_of(0, c)
            start = a * wide[:, 0:BLOCK] + c_ * wide[:, BLOCK : 2 * BLOCK] + d * wide[:, 2 * BLOCK :]
            current.append(start + jnp.where(eye, u, 0.0))
        for step in range(1, steps):
            stacked = jnp.concatenate([m.astype(BF16) for m in current], axis=0)
            terms = dot(stacked, weight)
            current = [
                advance(m, terms[k * BLOCK : (k + 1) * BLOCK], rows_of(step, c))
                for k, (m, c) in enumerate(zip(current, members))
            ]
        for m, c in zip(current, members):
            maps_ref[c, 0:BLOCK, :] = m


def scan_chunks(par_ref, weight, maps_ref, send_ref, chunks, steps, entry=None):
    eye = diagonal_mask()
    double = jnp.concatenate([weight, weight], axis=0)
    vector = par_ref[4, 0:chunks, :]
    if entry is not None:
        vector = jnp.concatenate([entry, jnp.zeros((chunks - 1, BLOCK), F32)], axis=0)
        vector = advance_rows(vector, double, par_ref, 0, chunks)
    for step in range(1, steps):
        vector = advance_rows(vector, double, par_ref, step * chunks, (step + 1) * chunks)
    pad = jnp.zeros((ROWS - BLOCK - 1, BLOCK), F32)
    for c in range(chunks):
        maps_ref[c, BLOCK:ROWS, :] = jnp.concatenate([vector[c : c + 1], pad], axis=0)
    width = 1
    while width < chunks:
        for left in range(width - 1, chunks, 2 * width):
            before = jnp.concatenate(split2(maps_ref[left]), axis=1)
            for right in range(left + 1, left + 1 + width):
                high, low = split2(maps_ref[right, 0:BLOCK, :])
                upper = jnp.concatenate([high, low], axis=1)
                under = jnp.concatenate([high, jnp.zeros_like(low)], axis=1)
                both = dot(before, jnp.concatenate([upper, under], axis=0))
                both = both[:, 0:BLOCK] + both[:, BLOCK:]
                maps_ref[right, 0:BLOCK, :] = both[0:BLOCK]
                maps_ref[right, BLOCK:ROWS, :] = both[BLOCK:] + maps_ref[right, BLOCK:ROWS, :]
        width *= 2
    matrix = maps_ref[chunks - 1, 0:BLOCK, :]
    diagonal = jnp.sum(jnp.where(eye, matrix, 0.0), axis=0, keepdims=True)
    tail = [p.astype(F32) for p in split3(diagonal)]
    tail += [p.astype(F32) for p in split3(maps_ref[chunks - 1, BLOCK : BLOCK + 1, :])]
    tail.append(jnp.zeros((ROWS - BLOCK - 6, BLOCK), F32))
    matrix = jnp.where(eye, 0.0, matrix).astype(BF16)
    tail = jnp.concatenate(tail, axis=0).astype(BF16)
    for peer in range(send_ref.shape[0]):
        send_ref[peer, 0:BLOCK, :] = matrix
        send_ref[peer, BLOCK:ROWS, :] = tail


def pack(
    index_ref, guess_hbm, proj_hbm, start_hbm, w_hbm, ub_hbm, cb_hbm,
    send_ref, w_ref, ub_ref, cb_ref, row_ref, guess_ref, proj_ref, start_ref, sems, *, blocks,
):
    own = pl.ds(pl.multiple_of(index_ref[1] * BLOCK, BLOCK), BLOCK)
    moves = (
        (guess_hbm, guess_ref),
        (proj_hbm, proj_ref),
        (start_hbm, start_ref),
        (w_hbm.at[:, :, own], w_ref),
        (ub_hbm.at[:, own], ub_ref),
        (cb_hbm.at[:, own], cb_ref),
    )
    copies = [
        pltpu.make_async_copy(source, target, sems.at[i])
        for i, (source, target) in enumerate(moves)
    ]
    for copy in copies:
        copy.start()
    for copy in copies[0:3]:
        copy.wait()
    steps = guess_ref.shape[0]
    high = guess_ref[...].astype(BF16).astype(F32)
    rest = guess_ref[...] - high
    start_high = start_ref[...].astype(BF16).astype(F32)
    start_rest = start_ref[...] - start_high
    inputs = (blocks + 1) * steps
    first = inputs + 3 * steps
    used = first + blocks + 1
    for target in range(blocks):
        lanes = slice(target * BLOCK, (target + 1) * BLOCK)
        for k in range(blocks):
            there = slice(k * BLOCK, (k + 1) * BLOCK)
            row_ref[target, k * steps : (k + 1) * steps, :] = high[:, there]
            row_ref[target, first + k : first + k + 1, :] = start_high[:, there]
        row_ref[target, blocks * steps : inputs, :] = rest[:, lanes]
        for g in range(3):
            begin = inputs + g * steps
            row_ref[target, begin : begin + steps, :] = proj_ref[g, :, lanes].astype(F32)
        row_ref[target, used - 1 : used, :] = start_rest[:, lanes]
        row_ref[target, used:, :] = jnp.zeros((row_ref.shape[1] - used, BLOCK), F32)
        packed = row_ref[target].astype(BF16)
        for far in range(send_ref.shape[0] // blocks):
            send_ref[far * blocks + target] = packed
    for copy in copies[3:]:
        copy.wait()


def first_maps(
    index_ref, own_ref, other_ref, w_ref, ub_ref, cb_ref,
    maps_ref, par_ref, prev_ref, guess_ref, proj_ref, rec_ref, row_ref,
    *, chunks, steps, blocks, stride,
):
    unit, place, group = index_ref[0], index_ref[1], index_ref[2]
    half = blocks * BLOCK
    inputs = (blocks + 1) * steps
    first = inputs + 3 * steps
    length = (chunks + 1) * stride
    total_steps = chunks * steps
    extra = 16

    def rows(side, start):
        return row_ref[pl.ds(side * length + start, chunks, stride=stride), :]

    def all_steps(side, start):
        return [rows(side, start + s) for s in range(steps)]

    def later(start):
        return [rows(0, start + s) for s in range(1, steps)] + [rows(0, stride + start)]

    def one(start, side=0):
        row = row_ref[pl.ds(side * length + start, 1), :]
        return jnp.broadcast_to(row, (extra, BLOCK))

    row_ref[length - stride : length, :] = jnp.zeros((stride, BLOCK), F32)
    total = 0.0
    for side, (ref, owner) in enumerate(((own_ref, unit), (other_ref, 1 - unit))):
        row_ref[side * length : side * length + chunks * stride, :] = ref[...].astype(F32)
        panels = [
            jnp.concatenate(all_steps(side, k * steps) + [one(first + k, side)], axis=0).astype(BF16)
            for k in range(blocks)
        ]
        weights = columns(w_ref, owner * half, half)
        total = total + dot(jnp.concatenate(panels, axis=1), weights)
    proj = []
    for g in range(3):
        start = inputs + g * steps
        proj.append(jnp.concatenate(later(start) + [one(start)], axis=0))
        proj_ref[g] = proj[g][0:total_steps]
    own, rest = place * steps, blocks * steps
    begin = one(first + place) + one(first + blocks)
    prev = jnp.concatenate(all_steps(0, own) + [begin], axis=0)
    prev += jnp.concatenate(all_steps(0, rest) + [jnp.zeros_like(begin)], axis=0)
    guess = jnp.concatenate(later(own) + [one(own)], axis=0)
    guess += jnp.concatenate(later(rest) + [one(rest)], axis=0)
    prev_ref[...] = prev[0:total_steps]
    guess_ref[...] = guess[0:total_steps]
    gates(total, proj, prev, guess, ub_ref, cb_ref, par_ref)
    entry = jnp.where(group == 0, par_ref[4, total_steps : total_steps + 1, :], 0.0)
    par_ref[4, total_steps : total_steps + 1, :] = entry
    rec_ref[...] = total[total_steps - chunks : total_steps]
    weight = columns(w_ref, (unit * blocks + place) * BLOCK, BLOCK)
    compose_chunks(par_ref, weight, maps_ref, 0, maps_ref.shape[0], chunks, steps)


def finish_maps(
    index_ref, next_ref, rec_ref, w_ref, ub_ref, cb_ref, some_ref, par_in, prev_ref, guess_in, proj_in,
    send_ref, maps_ref, par_ref, guess_ref, proj_ref, row_ref,
    *, chunks, steps, blocks,
):
    unit, place = index_ref[0], index_ref[1]
    total_steps = chunks * steps
    low = total_steps - chunks
    done = some_ref.shape[0]
    inputs = (blocks + 1) * steps
    row_ref[...] = next_ref[...].astype(F32)
    last = lax.broadcasted_iota(jnp.int32, (chunks, BLOCK), 0) == chunks - 1

    def row(start):
        return row_ref[pl.ds(start, 1), :]

    par_ref[...] = par_in[...]
    guess_ref[...] = guess_in[...]
    proj_ref[...] = proj_in[...]
    proj = []
    for g in range(3):
        proj.append(jnp.where(last, row(inputs + g * steps), proj_in[g, low:total_steps, :]))
        proj_ref[g, low:total_steps, :] = proj[g]
    guess = row(place * steps) + row(blocks * steps)
    guess = jnp.where(last, guess, guess_in[low:total_steps, :])
    guess_ref[low:total_steps, :] = guess
    prev = prev_ref[low:total_steps, :]
    gates(rec_ref[...], proj, prev, guess, ub_ref, cb_ref, par_ref, low)
    weight = columns(w_ref, (unit * blocks + place) * BLOCK, BLOCK)
    compose_chunks(par_ref, weight, maps_ref, done, chunks, chunks, steps)
    for c in range(done):
        maps_ref[c, 0:BLOCK, :] = some_ref[c]
    entry = par_in[4, total_steps : total_steps + 1, :]
    scan_chunks(par_ref, weight, maps_ref, send_ref, chunks, steps, entry)


def next_maps(
    index_ref, panel_ref, proj_ref, prev_ref, guess_ref, w_ref, ub_ref, cb_ref,
    send_ref, maps_ref, par_ref, *, chunks, steps, blocks,
):
    unit, place = index_ref[0], index_ref[1]
    sides = panel_ref.shape[0] // blocks
    panels = [panel_ref[k * sides + side] for side in range(sides) for k in range(blocks)]
    total = dot(jnp.concatenate(panels, axis=1), columns(w_ref, 0, w_ref.shape[1]))
    gates(total, proj_ref, prev_ref[...], guess_ref[...], ub_ref, cb_ref, par_ref)
    weight = columns(w_ref, (unit * blocks + place) * BLOCK, BLOCK)
    compose_chunks(par_ref, weight, maps_ref, 0, chunks, chunks, steps)
    scan_chunks(par_ref, weight, maps_ref, send_ref, chunks, steps)


def solve(index_ref, got_ref, maps_ref, par_ref, w_ref, chunks, steps, blocks, entry=0.0):
    unit, place, group = index_ref[0], index_ref[1], index_ref[2]

    def pass_group(k, delta):
        block = got_ref[k]
        matrix = block[0:BLOCK]
        tail = block[BLOCK:ROWS].astype(F32)
        diagonal = tail[0:1] + tail[1:2] + tail[2:3]
        vector = tail[3:4] + tail[4:5] + tail[5:6]
        terms = dot(
            jnp.concatenate(split2(delta), axis=1), jnp.concatenate([matrix, matrix], axis=0)
        )
        return terms + delta * diagonal + vector

    delta = lax.fori_loop(0, group, pass_group, jnp.zeros((16, BLOCK), F32))
    column = jnp.transpose(jnp.broadcast_to(delta[0:1], (BLOCK, BLOCK)))
    entries = [delta[0:1] + entry]
    for c in range(chunks - 1):
        through = jnp.sum(column * maps_ref[c, 0:BLOCK, :], axis=0, keepdims=True)
        entries.append(through + maps_ref[c, BLOCK : BLOCK + 1, :])
    entries = jnp.concatenate(entries, axis=0)
    weight = columns(w_ref, (unit * blocks + place) * BLOCK, BLOCK)
    double = jnp.concatenate([weight, weight], axis=0)
    current, after = entries, []
    for step in range(steps):
        current = advance_rows(current, double, par_ref, step * chunks, (step + 1) * chunks)
        after.append(current)
    return entries, after


def first_states(
    index_ref, got_ref, maps_ref, par_ref, w_ref, prev_ref, guess_ref,
    send_ref, prev_out, guess_out, *, chunks, steps, blocks,
):
    entry = par_ref[4, chunks * steps : chunks * steps + 1, :]
    entries, after = solve(
        index_ref, got_ref, maps_ref, par_ref, w_ref, chunks, steps, blocks, entry
    )
    prev = prev_ref[...] + jnp.concatenate([entries] + after[:-1], axis=0)
    prev_out[...] = prev
    guess_out[...] = guess_ref[...] + jnp.concatenate(after, axis=0)
    panel = prev.astype(BF16)
    for peer in range(send_ref.shape[0]):
        send_ref[peer] = panel


def last_states(
    index_ref, got_ref, maps_ref, par_ref, w_ref, prev_ref,
    send_ref, state_ref, *, chunks, steps, blocks,
):
    quarter = index_ref[3]
    entries, after = solve(index_ref, got_ref, maps_ref, par_ref, w_ref, chunks, steps - 1, blocks)
    state_ref[...] = prev_ref[...] + jnp.concatenate([entries] + after, axis=0)
    near = send_ref.shape[0]
    for peer in range(near):
        for step in range(steps):
            row = step * chunks + quarter * near + peer
            send_ref[peer, step : step + 1, :] = state_ref[pl.ds(row, 1), :]


SMEM = pl.BlockSpec(memory_space=pltpu.SMEM)
VMEM = pl.BlockSpec(memory_space=pltpu.VMEM)


def call(
    body, outs, args, scratch=(), first=SMEM, rest=VMEM, limit=24 * 1024 * 1024, cost=None
):
    return pl.pallas_call(
        body,
        out_shape=[jax.ShapeDtypeStruct(shape, kind) for shape, kind in outs],
        in_specs=[first] + [rest] * (len(args) - 1),
        out_specs=[VMEM] * len(outs),
        scratch_shapes=list(scratch),
        compiler_params=pltpu.CompilerParams(vmem_limit_bytes=limit),
        cost_estimate=cost,
        interpret=INTERPRET,
    )(*args)


def shards(projections, recurrent, update_bias, candidate_bias, start_state, initial_guess):
    _, steps, _, width_dev = projections.shape
    full_width = recurrent.shape[0]
    blocks = width_dev // BLOCK
    chunks = lax.axis_size(Z)
    near = lax.axis_size("zl")
    sides = lax.axis_size("unit")
    groups = lax.axis_size("x")
    total_steps = chunks * steps
    place = lax.axis_index("zl")
    unit = lax.axis_index("unit")
    group = lax.axis_index("x")
    index = jnp.stack([unit, place, group, lax.axis_index("zh")]).astype(jnp.int32)

    stride = -(-((blocks + 1) * (steps + 1) + 3 * steps) // 8) * 8
    far = [
        pltpu.with_memory_space_constraint(value, pltpu.HBM)
        for value in (
            initial_guess[0],
            jnp.transpose(projections[0], (1, 0, 2)),
            start_state,
            jnp.transpose(recurrent, (1, 0, 2)),
            update_bias[None],
            candidate_bias[None],
        )
    ]
    payload, weight, bias_u, bias_c = call(
        functools.partial(pack, blocks=blocks),
        [
            ((chunks, stride, BLOCK), BF16),
            ((3, full_width, BLOCK), BF16),
            ((1, BLOCK), F32),
            ((1, BLOCK), F32),
        ],
        (index, *far),
        [
            pltpu.VMEM((blocks, stride, BLOCK), F32),
            pltpu.VMEM((steps, width_dev), F32),
            pltpu.VMEM((3, steps, width_dev), BF16),
            pltpu.VMEM((1, width_dev), F32),
            pltpu.SemaphoreType.DMA((len(far),)),
        ],
        rest=pl.BlockSpec(memory_space=pltpu.HBM),
    )
    own = lax.all_to_all(payload, Z, split_axis=0, concat_axis=0, tiled=True)
    after = lax.ppermute(own[0], "x", [(k + 1, k) for k in range(groups - 1)])
    other = lax.ppermute(own, "unit", [(s, sides - 1 - s) for s in range(sides)])
    own = own.reshape(chunks * stride, BLOCK)
    other = other.reshape(chunks * stride, BLOCK)

    sizes = dict(chunks=chunks, steps=steps, blocks=blocks)
    maps_out = [
        ((groups, ROWS, BLOCK), BF16),
        ((chunks, ROWS, BLOCK), F32),
        ((5, total_steps, BLOCK), F32),
    ]
    rows_out = [((total_steps, BLOCK), F32)] * 2
    params_out = [((5, total_steps + 16, BLOCK), F32)]
    proj_out = [((3, total_steps, BLOCK), F32)]
    some, params, prev, guess, proj, rec = call(
        functools.partial(first_maps, stride=stride, **sizes),
        [((chunks - PART, BLOCK, BLOCK), F32)]
        + params_out
        + rows_out
        + proj_out
        + [((chunks, 3 * BLOCK), F32)],
        (index, own, other, weight, bias_u, bias_c),
        [pltpu.VMEM((sides * (chunks + 1) * stride, BLOCK), F32)],
        cost=pl.CostEstimate(flops=4 * 10**9, bytes_accessed=4 * 10**6, transcendentals=0),
    )
    send, maps, params, guess, proj = call(
        functools.partial(finish_maps, **sizes),
        maps_out[:2] + params_out + rows_out[:1] + proj_out,
        (index, after, rec, weight, bias_u, bias_c, some, params, prev, guess, proj),
        [pltpu.VMEM((stride, BLOCK), F32)],
    )
    got = lax.all_to_all(send, "x", split_axis=0, concat_axis=0, tiled=True)
    send, prev, guess = call(
        functools.partial(first_states, **sizes),
        [((near * sides, total_steps, BLOCK), BF16)] + rows_out,
        (index, got, maps, params, weight, prev, guess),
    )
    panels = lax.all_to_all(send, ("zl", "unit"), split_axis=0, concat_axis=0, tiled=True)
    send, maps, params = call(
        functools.partial(next_maps, **sizes),
        maps_out,
        (index, panels, proj, prev, guess, weight, bias_u, bias_c),
    )
    got = lax.all_to_all(send, "x", split_axis=0, concat_axis=0, tiled=True)
    (send,) = call(
        functools.partial(last_states, **sizes),
        [((near, steps, BLOCK), F32)],
        (index, got, maps, params, weight, prev),
        [pltpu.VMEM((total_steps, BLOCK), F32)],
    )
    final = lax.all_to_all(send, "zl", split_axis=0, concat_axis=0, tiled=True)
    return jnp.transpose(final, (1, 0, 2)).reshape(1, steps, width_dev)


def solution(mesh):
    count = mesh.shape["tm"]
    near = 4
    finer = Mesh(
        mesh.devices.reshape(
            mesh.shape["sweep"], GROUPS, count // GROUPS // near, near, mesh.shape["unit"]
        ),
        ("sweep", "x", "zh", "zl", "unit"),
    )
    return jax.shard_map(
        shards,
        mesh=finer,
        in_specs=(
            P("sweep", TM, None, "unit"),
            P("sweep", None, "unit"),
            P(("sweep", "unit")),
            P(("sweep", "unit")),
            P("sweep", "unit"),
            P("sweep", TM, "unit"),
        ),
        out_specs=P("sweep", TM, "unit"),
        check_vma=False,
    )
```

```python
import functools

import jax
import jax.numpy as jnp
from jax import lax
from jax.experimental import pallas as pl
from jax.experimental.pallas import tpu as pltpu
from jax.sharding import Mesh
from jax.sharding import PartitionSpec as P

BLOCK = 128
GROUPS = 8
TM = ("x", "zh", "zl")
Z = ("zh", "zl")
INTERPRET = False
ROWS = BLOCK + 16
SENT = BLOCK + 8
F32 = jnp.float32
BF16 = jnp.bfloat16


def split2(value):
    high = value.astype(BF16)
    low = (value - high.astype(F32)).astype(BF16)
    return high, low


def split3(value):
    high = value.astype(BF16)
    rest = value - high.astype(F32)
    mid = rest.astype(BF16)
    low = (rest - mid.astype(F32)).astype(BF16)
    return high, mid, low


def dot(left, right):
    return jnp.dot(left, right, preferred_element_type=F32)


def columns(w_ref, begin, count):
    begin = pl.multiple_of(begin, BLOCK)
    return jnp.concatenate([w_ref[g, pl.ds(begin, count), :] for g in range(3)], axis=1)


def gates(rec, proj, prev, guess, ub_ref, cb_ref, par_ref, low=0):
    update = jax.nn.sigmoid(proj[0] + rec[:, 0:BLOCK] + ub_ref[...])
    reset = jax.nn.sigmoid(proj[1] + rec[:, BLOCK : 2 * BLOCK])
    inner = rec[:, 2 * BLOCK : 3 * BLOCK] + cb_ref[...]
    cand = jnp.tanh(proj[2] + reset * inner)
    mapped = (1.0 - update) * cand + update * prev
    full = (1.0 - update) * (1.0 - cand * cand) * reset
    high = low + rec.shape[0]
    par_ref[0, low:high] = update
    par_ref[1, low:high] = (prev - cand) * update * (1.0 - update)
    par_ref[2, low:high] = full * inner * (1.0 - reset)
    par_ref[3, low:high] = full
    par_ref[4, low:high] = mapped - guess


def advance(value, terms, rows):
    u, a, c, d = rows
    return (
        u * value
        + a * terms[:, 0:BLOCK]
        + c * terms[:, BLOCK : 2 * BLOCK]
        + d * terms[:, 2 * BLOCK : 3 * BLOCK]
    )


def advance_rows(value, double, par_ref, low, high):
    terms = dot(jnp.concatenate(split2(value), axis=1), double)
    rows = [par_ref[i, low:high, :] for i in range(4)]
    return advance(value, terms, rows) + par_ref[4, low:high, :]


PART = 4


def diagonal_mask():
    shape = (BLOCK, BLOCK)
    return lax.broadcasted_iota(jnp.int32, shape, 0) == lax.broadcasted_iota(jnp.int32, shape, 1)


def compose_chunks(par_ref, weight, maps_ref, begin, end, chunks, steps):
    eye = diagonal_mask()
    wide = weight.astype(F32)
    for first in range(begin, end, PART):
        members = range(first, first + PART)

        def rows_of(step, c):
            return [par_ref[i, step * chunks + c : step * chunks + c + 1, :] for i in range(4)]

        current = []
        for c in members:
            u, a, c_, d = rows_of(0, c)
            start = a * wide[:, 0:BLOCK] + c_ * wide[:, BLOCK : 2 * BLOCK] + d * wide[:, 2 * BLOCK :]
            current.append(start + jnp.where(eye, u, 0.0))
        for step in range(1, steps):
            stacked = jnp.concatenate([m.astype(BF16) for m in current], axis=0)
            terms = dot(stacked, weight)
            current = [
                advance(m, terms[k * BLOCK : (k + 1) * BLOCK], rows_of(step, c))
                for k, (m, c) in enumerate(zip(current, members))
            ]
        for m, c in zip(current, members):
            maps_ref[c, 0:BLOCK, :] = m


def add_vectors(par_ref, weight, maps_ref, begin, end, chunks, steps, entry=None):
    double = jnp.concatenate([weight, weight], axis=0)
    vector = par_ref[4, 0:chunks, :]
    if entry is not None:
        vector = jnp.concatenate([entry, jnp.zeros((chunks - 1, BLOCK), F32)], axis=0)
        vector = advance_rows(vector, double, par_ref, 0, chunks)
    for step in range(1, steps):
        vector = advance_rows(vector, double, par_ref, step * chunks, (step + 1) * chunks)
    pad = jnp.zeros((ROWS - BLOCK - 1, BLOCK), F32)
    for c in range(begin, end):
        maps_ref[c, BLOCK:ROWS, :] = jnp.concatenate([vector[c : c + 1], pad], axis=0)


def scan(maps_ref, begin, end, width, limit):
    while width < limit:
        for left in range(begin + width - 1, end, 2 * width):
            before = jnp.concatenate(split2(maps_ref[left]), axis=1)
            for right in range(left + 1, left + 1 + width):
                high, low = split2(maps_ref[right, 0:BLOCK, :])
                upper = jnp.concatenate([high, low], axis=1)
                under = jnp.concatenate([high, jnp.zeros_like(low)], axis=1)
                both = dot(before, jnp.concatenate([upper, under], axis=0))
                both = both[:, 0:BLOCK] + both[:, BLOCK:]
                maps_ref[right, 0:BLOCK, :] = both[0:BLOCK]
                maps_ref[right, BLOCK:ROWS, :] = both[BLOCK:] + maps_ref[right, BLOCK:ROWS, :]
        width *= 2


def send_map(maps_ref, send_ref, chunks):
    eye = diagonal_mask()
    matrix = maps_ref[chunks - 1, 0:BLOCK, :]
    diagonal = jnp.sum(jnp.where(eye, matrix, 0.0), axis=0, keepdims=True)
    tail = [p.astype(F32) for p in split3(diagonal)]
    tail += [p.astype(F32) for p in split3(maps_ref[chunks - 1, BLOCK : BLOCK + 1, :])]
    tail.append(jnp.zeros((SENT - BLOCK - 6, BLOCK), F32))
    matrix = jnp.where(eye, 0.0, matrix).astype(BF16)
    tail = jnp.concatenate(tail, axis=0).astype(BF16)
    for peer in range(send_ref.shape[0]):
        send_ref[peer, 0:BLOCK, :] = matrix
        send_ref[peer, BLOCK:SENT, :] = tail


def pack(
    index_ref, guess_hbm, proj_hbm, start_hbm, w_hbm, ub_hbm, cb_hbm,
    send_ref, w_ref, ub_ref, cb_ref, row_ref, guess_ref, proj_ref, start_ref, sems, *, blocks,
):
    own = pl.ds(pl.multiple_of(index_ref[1] * BLOCK, BLOCK), BLOCK)
    moves = (
        (guess_hbm, guess_ref),
        (proj_hbm, proj_ref),
        (start_hbm, start_ref),
        (w_hbm.at[:, :, own], w_ref),
        (ub_hbm.at[:, own], ub_ref),
        (cb_hbm.at[:, own], cb_ref),
    )
    copies = [
        pltpu.make_async_copy(source, target, sems.at[i])
        for i, (source, target) in enumerate(moves)
    ]
    for copy in copies:
        copy.start()
    for copy in copies[0:3]:
        copy.wait()
    steps = guess_ref.shape[0]
    high = guess_ref[...].astype(BF16).astype(F32)
    rest = guess_ref[...] - high
    start_high = start_ref[...].astype(BF16).astype(F32)
    start_rest = start_ref[...] - start_high
    inputs = (blocks + 1) * steps
    first = inputs + 3 * steps
    used = first + blocks + 1
    for target in range(blocks):
        lanes = slice(target * BLOCK, (target + 1) * BLOCK)
        for k in range(blocks):
            there = slice(k * BLOCK, (k + 1) * BLOCK)
            row_ref[target, k * steps : (k + 1) * steps, :] = high[:, there]
            row_ref[target, first + k : first + k + 1, :] = start_high[:, there]
        row_ref[target, blocks * steps : inputs, :] = rest[:, lanes]
        for g in range(3):
            begin = inputs + g * steps
            row_ref[target, begin : begin + steps, :] = proj_ref[g, :, lanes].astype(F32)
        row_ref[target, used - 1 : used, :] = start_rest[:, lanes]
        row_ref[target, used:, :] = jnp.zeros((row_ref.shape[1] - used, BLOCK), F32)
        packed = row_ref[target].astype(BF16)
        for far in range(send_ref.shape[0] // blocks):
            send_ref[far * blocks + target] = packed
    for copy in copies[3:]:
        copy.wait()


def first_maps(
    index_ref, own_ref, other_ref, w_ref, ub_ref, cb_ref,
    maps_ref, par_ref, prev_ref, guess_ref, proj_ref, rec_ref, row_ref,
    *, chunks, steps, blocks, stride,
):
    unit, place, group = index_ref[0], index_ref[1], index_ref[2]
    half = blocks * BLOCK
    inputs = (blocks + 1) * steps
    first = inputs + 3 * steps
    length = (chunks + 1) * stride
    total_steps = chunks * steps
    extra = 16

    def rows(side, start):
        return row_ref[pl.ds(side * length + start, chunks, stride=stride), :]

    def all_steps(side, start):
        return [rows(side, start + s) for s in range(steps)]

    def later(start):
        return [rows(0, start + s) for s in range(1, steps)] + [rows(0, stride + start)]

    def one(start, side=0):
        row = row_ref[pl.ds(side * length + start, 1), :]
        return jnp.broadcast_to(row, (extra, BLOCK))

    row_ref[length - stride : length, :] = jnp.zeros((stride, BLOCK), F32)
    total = 0.0
    for side, (ref, owner) in enumerate(((own_ref, unit), (other_ref, 1 - unit))):
        row_ref[side * length : side * length + chunks * stride, :] = ref[...].astype(F32)
        panels = [
            jnp.concatenate(all_steps(side, k * steps) + [one(first + k, side)], axis=0).astype(BF16)
            for k in range(blocks)
        ]
        weights = columns(w_ref, owner * half, half)
        total = total + dot(jnp.concatenate(panels, axis=1), weights)
    proj = []
    for g in range(3):
        start = inputs + g * steps
        proj.append(jnp.concatenate(later(start) + [one(start)], axis=0))
        proj_ref[g] = proj[g][0:total_steps]
    own, rest = place * steps, blocks * steps
    begin = one(first + place) + one(first + blocks)
    prev = jnp.concatenate(all_steps(0, own) + [begin], axis=0)
    prev += jnp.concatenate(all_steps(0, rest) + [jnp.zeros_like(begin)], axis=0)
    guess = jnp.concatenate(later(own) + [one(own)], axis=0)
    guess += jnp.concatenate(later(rest) + [one(rest)], axis=0)
    prev_ref[...] = prev[0:total_steps]
    guess_ref[...] = guess[0:total_steps]
    gates(total, proj, prev, guess, ub_ref, cb_ref, par_ref)
    entry = jnp.where(group == 0, par_ref[4, total_steps : total_steps + 1, :], 0.0)
    par_ref[4, total_steps : total_steps + 1, :] = entry
    rec_ref[...] = total[total_steps - chunks : total_steps]
    weight = columns(w_ref, (unit * blocks + place) * BLOCK, BLOCK)
    done = maps_ref.shape[0]
    compose_chunks(par_ref, weight, maps_ref, 0, done, chunks, steps)
    add_vectors(par_ref, weight, maps_ref, 0, done, chunks, steps, entry)
    scan(maps_ref, 0, done, 1, PART)


def finish_maps(
    index_ref, next_ref, rec_ref, w_ref, ub_ref, cb_ref, some_ref, par_in, prev_ref, guess_in, proj_in,
    send_ref, maps_ref, par_ref, guess_ref, proj_ref, row_ref,
    *, chunks, steps, blocks,
):
    unit, place = index_ref[0], index_ref[1]
    total_steps = chunks * steps
    low = total_steps - chunks
    done = some_ref.shape[0]
    inputs = (blocks + 1) * steps
    row_ref[...] = next_ref[...].astype(F32)
    last = lax.broadcasted_iota(jnp.int32, (chunks, BLOCK), 0) == chunks - 1

    def row(start):
        return row_ref[pl.ds(start, 1), :]

    par_ref[...] = par_in[...]
    guess_ref[...] = guess_in[...]
    proj_ref[...] = proj_in[...]
    proj = []
    for g in range(3):
        proj.append(jnp.where(last, row(inputs + g * steps), proj_in[g, low:total_steps, :]))
        proj_ref[g, low:total_steps, :] = proj[g]
    guess = row(place * steps) + row(blocks * steps)
    guess = jnp.where(last, guess, guess_in[low:total_steps, :])
    guess_ref[low:total_steps, :] = guess
    prev = prev_ref[low:total_steps, :]
    gates(rec_ref[...], proj, prev, guess, ub_ref, cb_ref, par_ref, low)
    weight = columns(w_ref, (unit * blocks + place) * BLOCK, BLOCK)
    compose_chunks(par_ref, weight, maps_ref, done, chunks, chunks, steps)
    for c in range(done):
        maps_ref[c] = some_ref[c]
    add_vectors(par_ref, weight, maps_ref, done, chunks, chunks, steps)
    scan(maps_ref, done, chunks, 1, PART)
    scan(maps_ref, 0, chunks, PART, chunks)
    send_map(maps_ref, send_ref, chunks)


def next_maps(
    index_ref, panel_ref, proj_ref, prev_ref, guess_ref, w_ref, ub_ref, cb_ref,
    send_ref, maps_ref, par_ref, *, chunks, steps, blocks,
):
    unit, place = index_ref[0], index_ref[1]
    sides = panel_ref.shape[0] // blocks
    panels = [panel_ref[k * sides + side] for side in range(sides) for k in range(blocks)]
    total = dot(jnp.concatenate(panels, axis=1), columns(w_ref, 0, w_ref.shape[1]))
    gates(total, proj_ref, prev_ref[...], guess_ref[...], ub_ref, cb_ref, par_ref)
    weight = columns(w_ref, (unit * blocks + place) * BLOCK, BLOCK)
    compose_chunks(par_ref, weight, maps_ref, 0, chunks, chunks, steps)
    add_vectors(par_ref, weight, maps_ref, 0, chunks, chunks, steps)
    scan(maps_ref, 0, chunks, 1, chunks)
    send_map(maps_ref, send_ref, chunks)


def solve(index_ref, got_ref, maps_ref, par_ref, w_ref, chunks, steps, blocks, entry=0.0):
    unit, place, group = index_ref[0], index_ref[1], index_ref[2]

    def pass_group(k, delta):
        block = got_ref[k]
        matrix = block[0:BLOCK]
        tail = block[BLOCK:SENT].astype(F32)
        diagonal = tail[0:1] + tail[1:2] + tail[2:3]
        vector = tail[3:4] + tail[4:5] + tail[5:6]
        terms = dot(
            jnp.concatenate(split2(delta), axis=1), jnp.concatenate([matrix, matrix], axis=0)
        )
        return terms + delta * diagonal + vector

    tail = got_ref[0][BLOCK:SENT].astype(F32)
    begin = jnp.where(group > 0, tail[3:4] + tail[4:5] + tail[5:6], 0.0)
    delta = lax.fori_loop(1, group, pass_group, jnp.broadcast_to(begin, (16, BLOCK)))
    column = jnp.transpose(jnp.broadcast_to(delta[0:1], (BLOCK, BLOCK)))
    entries = [delta[0:1] + entry]
    for c in range(chunks - 1):
        through = jnp.sum(column * maps_ref[c, 0:BLOCK, :], axis=0, keepdims=True)
        entries.append(through + maps_ref[c, BLOCK : BLOCK + 1, :])
    entries = jnp.concatenate(entries, axis=0)
    weight = columns(w_ref, (unit * blocks + place) * BLOCK, BLOCK)
    double = jnp.concatenate([weight, weight], axis=0)
    current, after = entries, []
    for step in range(steps):
        current = advance_rows(current, double, par_ref, step * chunks, (step + 1) * chunks)
        after.append(current)
    return entries, after


def first_states(
    index_ref, got_ref, maps_ref, par_ref, w_ref, prev_ref, guess_ref,
    send_ref, prev_out, guess_out, *, chunks, steps, blocks,
):
    entry = par_ref[4, chunks * steps : chunks * steps + 1, :]
    entries, after = solve(
        index_ref, got_ref, maps_ref, par_ref, w_ref, chunks, steps, blocks, entry
    )
    prev = prev_ref[...] + jnp.concatenate([entries] + after[:-1], axis=0)
    prev_out[...] = prev
    guess_out[...] = guess_ref[...] + jnp.concatenate(after, axis=0)
    panel = prev.astype(BF16)
    for peer in range(send_ref.shape[0]):
        send_ref[peer] = panel


def last_states(
    index_ref, got_ref, maps_ref, par_ref, w_ref, prev_ref,
    send_ref, state_ref, *, chunks, steps, blocks,
):
    quarter = index_ref[3]
    entries, after = solve(index_ref, got_ref, maps_ref, par_ref, w_ref, chunks, steps - 1, blocks)
    state_ref[...] = prev_ref[...] + jnp.concatenate([entries] + after, axis=0)
    near = send_ref.shape[0]
    for peer in range(near):
        for step in range(steps):
            row = step * chunks + quarter * near + peer
            send_ref[peer, step : step + 1, :] = state_ref[pl.ds(row, 1), :]


SMEM = pl.BlockSpec(memory_space=pltpu.SMEM)
VMEM = pl.BlockSpec(memory_space=pltpu.VMEM)


def call(
    body, outs, args, scratch=(), first=SMEM, rest=VMEM, limit=24 * 1024 * 1024, cost=None
):
    return pl.pallas_call(
        body,
        out_shape=[jax.ShapeDtypeStruct(shape, kind) for shape, kind in outs],
        in_specs=[first] + [rest] * (len(args) - 1),
        out_specs=[VMEM] * len(outs),
        scratch_shapes=list(scratch),
        compiler_params=pltpu.CompilerParams(vmem_limit_bytes=limit),
        cost_estimate=cost,
        interpret=INTERPRET,
    )(*args)


def shards(projections, recurrent, update_bias, candidate_bias, start_state, initial_guess):
    _, steps, _, width_dev = projections.shape
    full_width = recurrent.shape[0]
    blocks = width_dev // BLOCK
    chunks = lax.axis_size(Z)
    near = lax.axis_size("zl")
    sides = lax.axis_size("unit")
    groups = lax.axis_size("x")
    total_steps = chunks * steps
    place = lax.axis_index("zl")
    unit = lax.axis_index("unit")
    group = lax.axis_index("x")
    index = jnp.stack([unit, place, group, lax.axis_index("zh")]).astype(jnp.int32)

    stride = -(-((blocks + 1) * (steps + 1) + 3 * steps) // 8) * 8
    far = [
        pltpu.with_memory_space_constraint(value, pltpu.HBM)
        for value in (
            initial_guess[0],
            jnp.transpose(projections[0], (1, 0, 2)),
            start_state,
            jnp.transpose(recurrent, (1, 0, 2)),
            update_bias[None],
            candidate_bias[None],
        )
    ]
    payload, weight, bias_u, bias_c = call(
        functools.partial(pack, blocks=blocks),
        [
            ((chunks, stride, BLOCK), BF16),
            ((3, full_width, BLOCK), BF16),
            ((1, BLOCK), F32),
            ((1, BLOCK), F32),
        ],
        (index, *far),
        [
            pltpu.VMEM((blocks, stride, BLOCK), F32),
            pltpu.VMEM((steps, width_dev), F32),
            pltpu.VMEM((3, steps, width_dev), BF16),
            pltpu.VMEM((1, width_dev), F32),
            pltpu.SemaphoreType.DMA((len(far),)),
        ],
        rest=pl.BlockSpec(memory_space=pltpu.HBM),
    )
    own = lax.all_to_all(payload, Z, split_axis=0, concat_axis=0, tiled=True)
    after = lax.ppermute(own[0], "x", [(k + 1, k) for k in range(groups - 1)])
    other = lax.ppermute(own, "unit", [(s, sides - 1 - s) for s in range(sides)])
    own = own.reshape(chunks * stride, BLOCK)
    other = other.reshape(chunks * stride, BLOCK)

    sizes = dict(chunks=chunks, steps=steps, blocks=blocks)
    maps_out = [
        ((groups, SENT, BLOCK), BF16),
        ((chunks, ROWS, BLOCK), F32),
        ((5, total_steps, BLOCK), F32),
    ]
    rows_out = [((total_steps, BLOCK), F32)] * 2
    params_out = [((5, total_steps + 16, BLOCK), F32)]
    proj_out = [((3, total_steps, BLOCK), F32)]
    some, params, prev, guess, proj, rec = call(
        functools.partial(first_maps, stride=stride, **sizes),
        [((chunks - PART, ROWS, BLOCK), F32)]
        + params_out
        + rows_out
        + proj_out
        + [((chunks, 3 * BLOCK), F32)],
        (index, own, other, weight, bias_u, bias_c),
        [pltpu.VMEM((sides * (chunks + 1) * stride, BLOCK), F32)],
        cost=pl.CostEstimate(flops=4 * 10**9, bytes_accessed=4 * 10**6, transcendentals=0),
    )
    send, maps, params, guess, proj = call(
        functools.partial(finish_maps, **sizes),
        maps_out[:2] + params_out + rows_out[:1] + proj_out,
        (index, after, rec, weight, bias_u, bias_c, some, params, prev, guess, proj),
        [pltpu.VMEM((stride, BLOCK), F32)],
    )
    got = lax.all_to_all(send, "x", split_axis=0, concat_axis=0, tiled=True)
    send, prev, guess = call(
        functools.partial(first_states, **sizes),
        [((near * sides, total_steps, BLOCK), BF16)] + rows_out,
        (index, got, maps, params, weight, prev, guess),
    )
    panels = lax.all_to_all(send, ("zl", "unit"), split_axis=0, concat_axis=0, tiled=True)
    send, maps, params = call(
        functools.partial(next_maps, **sizes),
        maps_out,
        (index, panels, proj, prev, guess, weight, bias_u, bias_c),
    )
    got = lax.all_to_all(send, "x", split_axis=0, concat_axis=0, tiled=True)
    (send,) = call(
        functools.partial(last_states, **sizes),
        [((near, steps, BLOCK), F32)],
        (index, got, maps, params, weight, prev),
        [pltpu.VMEM((total_steps, BLOCK), F32)],
    )
    final = lax.all_to_all(send, "zl", split_axis=0, concat_axis=0, tiled=True)
    return jnp.transpose(final, (1, 0, 2)).reshape(1, steps, width_dev)


def solution(mesh):
    count = mesh.shape["tm"]
    near = 4
    finer = Mesh(
        mesh.devices.reshape(
            mesh.shape["sweep"], GROUPS, count // GROUPS // near, near, mesh.shape["unit"]
        ),
        ("sweep", "x", "zh", "zl", "unit"),
    )
    return jax.shard_map(
        shards,
        mesh=finer,
        in_specs=(
            P("sweep", TM, None, "unit"),
            P("sweep", None, "unit"),
            P(("sweep", "unit")),
            P(("sweep", "unit")),
            P("sweep", "unit"),
            P("sweep", TM, "unit"),
        ),
        out_specs=P("sweep", TM, "unit"),
        check_vma=False,
    )
```
